32 devices in a mesh: fsdp: 8 (over z, x), ctx: 2 (over y), tp: 2 (over core).
Axes of the slice: x: 2, y: 2, z: 4, core: 2. Of those that a mesh axis runs over, the one named last changes fastest.
Arguments:
- hidden_in: bfloat16 [1024, 8, 768], P('ctx', 'fsdp'), may hold values from -6 to 6
- first_values: bfloat16 [1024, 8, 384], P('ctx', 'fsdp', 'tp'), may hold values from -6 to 6
- span_table: int32 [2, 2], replicated, may hold values from 0 to 3, as said below
- w_query: bfloat16 [768, 768], P('fsdp', 'tp'), may hold values from -0.21875 to 0.21875
- w_key: bfloat16 [768, 768], P('fsdp', 'tp'), may hold values from -0.21875 to 0.21875
- w_value: bfloat16 [768, 384], P('fsdp', 'tp'), may hold values from -0.21875 to 0.21875
- w_out: bfloat16 [768, 768], P('fsdp', 'tp'), may hold values from -3 to 3
- w_up: bfloat16 [768, 3072], P('fsdp', 'tp'), may hold values from -0.21875 to 0.21875
- w_down: bfloat16 [768, 3072], P('fsdp', 'tp'), may hold values from -0.109375 to 0.109375
- gain_attn: bfloat16 [768], P('fsdp'), may hold values from 0.5 to 1.5
- shift_attn: bfloat16 [768], P('fsdp'), may hold values from -1.5 to 1.5
- gain_mlp: bfloat16 [768], P('fsdp'), may hold values from 0.5 to 1.5
- shift_mlp: bfloat16 [768], P('fsdp'), may hold values from -1.5 to 1.5
- cotangent: bfloat16 [1024, 8, 768], P('ctx', 'fsdp'), may hold values from -6 to 6
Outputs:
- out_hidden: float32 [1024, 8, 768], P('ctx', 'fsdp')
- grad_hidden: float32 [1024, 8, 768], P('ctx', 'fsdp')
- grad_first: float32 [1024, 8, 384], P('ctx', 'fsdp', 'tp')
- grad_query: float32 [768, 768], P('fsdp', 'tp')
- grad_key: float32 [768, 768], P('fsdp', 'tp')
- grad_value: float32 [768, 384], P('fsdp', 'tp')
- grad_outproj: float32 [768, 768], P('fsdp', 'tp')
- grad_up: float32 [768, 3072], P('fsdp', 'tp')
- grad_down: float32 [768, 3072], P('fsdp', 'tp')
- grad_gain_attn: float32 [768], P('fsdp')
- grad_shift_attn: float32 [768], P('fsdp')
- grad_gain_mlp: float32 [768], P('fsdp')
- grad_shift_mlp: float32 [768], P('fsdp')
The draws below stay inside these ranges and needn't reach their ends.
Inputs may be any that keep to these rules, and one draw needn't show every extreme that they name: `span_table`: every span number appears exactly once in the table.
All inputs are finite; a program needn't handle non-finite values.
Results may differ from the reference program's by a relative error of at most 0.02.
Values may be sent and summed in bfloat16 or wider, within the bound.
No kernel may reach another device: no remote copies, remote signals or barrier semaphores. Data moves between devices by JAX's collectives and lax.ppermute only.
A program may use at most 128 MiB of HBM per device.

```python
import jax
import jax.numpy as jnp
from jax import lax

D = 768
FF = 3072
HEADS = 12
HEAD_DIM = 64
FRESH = 6
SPAN = 256
SEQ_LEN = 1024
BATCH = 8
N_CTX = 2


def draw_span_table(key, part):
    order = jax.random.permutation(jax.random.fold_in(key, 11), 2 * N_CTX).astype(jnp.int32)
    return order.reshape(N_CTX, 2).astype(jnp.int32)


def shard_levels(stream_key, shape, cuts, low, largest):
    loudness, own = 1.0, jax.random.fold_in(stream_key, 6)
    for dim, shards_of in cuts:
        steps = jnp.exp(jax.random.uniform(jax.random.fold_in(own, dim), (shards_of,), jnp.float32, low / len(cuts), largest / len(cuts)))
        loudness = loudness * jnp.repeat(steps, shape[dim] // shards_of).reshape([-1 if axis == dim else 1 for axis in range(len(shape))])
    return loudness


def noise(key, shape, scale, most, shards=(), held_as=jnp.bfloat16):
    level = shard_levels(key, shape, shards, -0.22, 0.18) if shards else 1.0
    values = jax.random.normal(key, shape, jnp.float32) * scale * level
    return jnp.minimum(jnp.maximum(values, -most), most).astype(held_as)


def setup_inputs(seed: int = 0) -> dict:
    seeds = jax.random.split(jax.random.key(seed), 15)
    return {
        "hidden_in": noise(seeds[0], (SEQ_LEN, BATCH, D), 1.0, 6.0, ((0, 2), (1, 8))),
        "first_values": noise(seeds[1], (SEQ_LEN, BATCH, FRESH * HEAD_DIM), 1.0, 6.0, ((0, 2), (1, 8), (2, 2))),
        "span_table": draw_span_table(jax.random.fold_in(seeds[14], 71), 0),
        "w_query": noise(seeds[3], (D, D), D ** -0.5, 0.21875, ((0, 8), (1, 2))),
        "w_key": noise(seeds[4], (D, D), D ** -0.5, 0.21875, ((0, 8), (1, 2))),
        "w_value": noise(seeds[5], (D, FRESH * HEAD_DIM), D ** -0.5, 0.21875, ((0, 8), (1, 2))),
        "w_out": noise(seeds[6], (D, D), 4 ** -0.5, 3.0, ((0, 8), (1, 2))),
        "w_up": noise(seeds[7], (D, FF), D ** -0.5, 0.21875, ((0, 8), (1, 2))),
        "w_down": noise(seeds[8], (D, FF), FF ** -0.5, 0.109375, ((0, 8), (1, 2))),
        "gain_attn": jnp.clip(1.0 + 0.1 * jax.random.normal(seeds[9], (D,), jnp.float32), 0.5, 1.5).astype(jnp.bfloat16),
        "shift_attn": noise(seeds[10], (D,), 0.3, 1.5, ((0, 8),)),
        "gain_mlp": jnp.clip(1.0 + 0.1 * jax.random.normal(seeds[11], (D,), jnp.float32), 0.5, 1.5).astype(jnp.bfloat16),
        "shift_mlp": noise(seeds[12], (D,), 0.3, 1.5, ((0, 8),)),
        "cotangent": noise(seeds[13], (SEQ_LEN, BATCH, D), 1.0, 6.0, ((0, 2), (1, 8))),
    }


@jax.custom_vjp
def low(v):
    return lax.optimization_barrier(v.astype(jnp.bfloat16)).astype(jnp.float32)

@jax.custom_vjp
def low_back(v):
    return v

def low_keep(v):
    return (low(v), None)

def low_pass(kept, grad):
    return (grad,)

def back_keep(v):
    return (v, None)

def back_low(kept, grad):
    return (low(grad),)
low.defvjp(low_keep, low_pass)
low_back.defvjp(back_keep, back_low)

def normalize(values, gain, shift):
    mean = lax.optimization_barrier(jnp.mean(values, axis=-1, keepdims=True))
    centred = values - mean
    spread = lax.optimization_barrier(jnp.mean(centred * centred, axis=-1, keepdims=True))
    return centred * lax.rsqrt(spread + 1e-05) * gain + shift

def gelu_tanh(values):
    return 0.5 * values * (1.0 + jnp.tanh(0.7978845608028654 * (values + 0.044715 * values * values * values)))

def attend(query, keys, values, places):
    block = min(512, SEQ_LEN)
    blocks = SEQ_LEN // block
    scale = HEAD_DIM ** (-0.5)

    def one_block(pair):
        q_block, p_block = pair
        scores = jnp.einsum('qhd,khd->hqk', q_block, keys, precision=lax.Precision.HIGHEST) * scale
        scores = low_back(scores)
        allowed = places[None, None, :] <= p_block[None, :, None]
        scores = jnp.where(allowed, scores, -1e+30)
        weights = low(jax.nn.softmax(scores, axis=-1))
        return jnp.einsum('hqk,khd->qhd', weights, values, precision=lax.Precision.HIGHEST)
    result = lax.map(jax.checkpoint(one_block), (query.reshape(blocks, block, HEADS, HEAD_DIM), places.reshape(blocks, block)))
    return result.reshape(SEQ_LEN, HEADS, HEAD_DIM)

def layer(hidden, first, places, params):
    w_query, w_key, w_value, w_out, w_up, w_down, gain_attn, shift_attn, gain_mlp, shift_mlp = params
    high = lax.Precision.HIGHEST
    h_one = low(normalize(hidden, gain_attn, shift_attn))
    query = low_back(low(jnp.dot(h_one, w_query, precision=high)))
    keys = low_back(low(jnp.dot(h_one, w_key, precision=high)))
    fresh = low_back(low(jnp.dot(h_one, w_value, precision=high)))
    values = jnp.stack([fresh.reshape(SEQ_LEN, FRESH, HEAD_DIM), first.reshape(SEQ_LEN, FRESH, HEAD_DIM)], axis=2).reshape(SEQ_LEN, HEADS, HEAD_DIM)
    mixed = attend(query.reshape(SEQ_LEN, HEADS, HEAD_DIM), keys.reshape(SEQ_LEN, HEADS, HEAD_DIM), values, places)
    mixed = low_back(low(mixed.reshape(SEQ_LEN, D)))
    branch = low_back(jnp.dot(mixed, w_out.T, precision=high))
    resid = hidden + branch
    h_two = low(normalize(resid, gain_mlp, shift_mlp))
    upper = low_back(jnp.dot(h_two, w_up, precision=high))
    act = low(gelu_tanh(upper))
    return resid + jnp.dot(act, w_down.T, precision=high)

def to_float(array):
    return array.astype(jnp.float32)

def reference(hidden_in, first_values, span_table, w_query, w_key, w_value, w_out, w_up, w_down, gain_attn, shift_attn, gain_mlp, shift_mlp, cotangent):
    places = (jnp.repeat(span_table.reshape(-1), SPAN) * SPAN + jnp.arange(SEQ_LEN, dtype=jnp.int32) % SPAN).astype(jnp.int32)
    params = jax.tree.map(to_float, (w_query, w_key, w_value, w_out, w_up, w_down, gain_attn, shift_attn, gain_mlp, shift_mlp))
    inputs = jnp.transpose(to_float(hidden_in), (1, 0, 2))
    firsts = jnp.transpose(to_float(first_values), (1, 0, 2))
    cotan = jnp.transpose(to_float(cotangent), (1, 0, 2))

    def seq_layer(hidden, first, weights):
        return layer(hidden, first, places, weights)
    saved_layer = jax.checkpoint(seq_layer)

    def forward(inputs_all, firsts_all, weights):

        def step(carry, pair):
            return (carry, saved_layer(pair[0], pair[1], weights))
        _, outputs = lax.scan(step, jnp.zeros((), jnp.float32), (inputs_all, firsts_all))
        return outputs
    outputs, pull = jax.vjp(forward, inputs, firsts, params)
    d_inputs, d_firsts, d_params = pull(cotan)
    return (jnp.transpose(outputs, (1, 0, 2)), jnp.transpose(d_inputs, (1, 0, 2)), jnp.transpose(d_firsts, (1, 0, 2)), d_params[0], d_params[1], d_params[2], d_params[3], d_params[4], d_params[5], d_params[6], d_params[7], d_params[8], d_params[9])
```

```python
import jax
import jax.numpy as jnp
from jax import lax
from jax.sharding import PartitionSpec as P

HEADS = 12
HEAD_DIM = 64
low = jnp.bfloat16
wide = jnp.float32


eps_norm = 1e-05
big_negative = -1e30
gelu_coef = 0.7978845608028654
cube_coef = 0.044715


def passed_along(value, axis, steps):
    count = lax.axis_size(axis)
    pairs = [(source, (source + steps) % count) for source in range(count)]
    return lax.ppermute(value, axis, pairs)


def normalize_rows(values):
    mean = jnp.mean(values, axis=-1, keepdims=True)
    centred = values - mean
    inverse = lax.rsqrt(jnp.mean(centred * centred, axis=-1, keepdims=True) + eps_norm)
    return (centred * inverse, inverse)


def normalize_back(d_norm, unit, inverse, gain):
    scaled = d_norm * gain
    inner = (
        scaled
        - jnp.mean(scaled, axis=-1, keepdims=True)
        - unit * jnp.mean(scaled * unit, axis=-1, keepdims=True)
    )
    return inverse * inner


def gelu_forward(values):
    return (
        0.5 * values * (1.0 + jnp.tanh(gelu_coef * (values + cube_coef * values * values * values)))
    )


def gelu_slope(values):
    tanh_val = jnp.tanh(gelu_coef * (values + cube_coef * values * values * values))
    return 0.5 * (1.0 + tanh_val) + 0.5 * values * (1.0 - tanh_val * tanh_val) * gelu_coef * (
        1.0 + 3.0 * cube_coef * values * values
    )


def contract_rows(left, right):
    return lax.dot_general(
        left, right, (((0,), (0,)), ((), ())), preferred_element_type=jnp.float32
    )


def contract_cols(left, right):
    return lax.dot_general(
        left, right, (((1,), (1,)), ((), ())), preferred_element_type=jnp.float32
    )


def block_scores(query, keys, q_places, k_places, scale):
    scores = jnp.einsum("qshe,kshe->shqk", query, keys, preferred_element_type=jnp.float32) * scale
    allowed = k_places[None, None, None, :] <= q_places[None, None, :, None]
    return (jnp.where(allowed, scores, big_negative), allowed)


def absorb_block(state, query, q_places, k_block, v_block, p_block, scale):
    top, total, summed = state
    scores, allowed = block_scores(query, k_block, q_places, p_block, scale)
    new_top = jnp.maximum(top, jnp.max(scores, axis=-1))
    factor = jnp.exp(top - new_top)
    weights = jnp.where(allowed, jnp.exp(scores - new_top[..., None]), 0.0)
    total = total * factor + jnp.sum(weights, axis=-1)
    update = jnp.einsum(
        "shqk,kshe->qshe", weights.astype(jnp.bfloat16), v_block, preferred_element_type=jnp.float32
    )
    summed = summed * jnp.transpose(factor, (2, 0, 1))[..., None] + update
    return (new_top, total, summed)


def make_absorb(query, q_places, places_all, scale):
    rows, seqs, heads, width = query.shape

    def absorb(carry, piece, start):
        keys, values = piece
        pairs = keys.shape[0] // rows
        k_pairs = keys.reshape(pairs, rows, seqs, heads, width)
        v_pairs = values.reshape(pairs, rows, seqs, heads, width)
        p_pairs = places_all.reshape(pairs, rows)

        def one_pair(state, item):
            k_pair, v_pair, p_pair = item
            return (absorb_block(state, query, q_places, k_pair, v_pair, p_pair, scale), None)

        carry, _ = lax.scan(one_pair, carry, (k_pairs, v_pairs, p_pairs))
        return carry

    return absorb


def grad_block(query, d_mixed, delta, log_total, q_places, k_block, v_block, p_block, scale):
    scores, allowed = block_scores(query, k_block, q_places, p_block, scale)
    weights = jnp.where(allowed, jnp.exp(scores - log_total[..., None]), 0.0)
    d_weights = jnp.einsum("qshe,kshe->shqk", d_mixed, v_block, preferred_element_type=jnp.float32)
    d_scores = (weights * (d_weights - delta[..., None])).astype(jnp.bfloat16)
    part_query = jnp.einsum(
        "shqk,kshe->qshe", d_scores, k_block, preferred_element_type=jnp.float32
    )
    part_key = jnp.einsum("shqk,qshe->kshe", d_scores, query, preferred_element_type=jnp.float32)
    part_value = jnp.einsum(
        "shqk,qshe->kshe", weights.astype(jnp.bfloat16), d_mixed, preferred_element_type=jnp.float32
    )
    return (part_query, part_key, part_value)


def grad_pair(query, d_mixed, delta, log_total, q_places, k_shard, v_shard, p_shard, scale):
    return grad_block(query, d_mixed, delta, log_total, q_places, k_shard, v_shard, p_shard, scale)


def local_ring(
    hidden_in,
    first_values,
    span_table,
    w_query,
    w_key,
    w_value,
    w_out,
    w_up,
    w_down,
    gain_attn,
    shift_attn,
    gain_mlp,
    shift_mlp,
    cotangent,
):
    rows, seqs, width = hidden_in.shape
    count = rows * seqs
    ranks = lax.axis_size("ctx")
    rank = lax.axis_index("ctx")
    span_rows = rows // 2
    local_heads = HEADS // lax.axis_size("tp")
    head_cols = local_heads * HEAD_DIM
    scale = HEAD_DIM ** (-0.5)
    places_all = (
        jnp.repeat(span_table.reshape(-1), span_rows) * span_rows
        + jnp.arange(ranks * rows, dtype=jnp.int32) % span_rows
    )
    q_places = lax.dynamic_slice_in_dim(places_all, rank * rows, rows)
    x_rows = hidden_in.reshape(count, width).astype(jnp.float32)
    unit_one, inverse_one = normalize_rows(x_rows)
    wq_full, wk_full, wv_full, wo_full, gain_one, shift_one = (
        lax.all_gather(w_query, "fsdp", axis=0, tiled=True),
        lax.all_gather(w_key, "fsdp", axis=0, tiled=True),
        lax.all_gather(w_value, "fsdp", axis=0, tiled=True),
        lax.all_gather(w_out, "fsdp", axis=0, tiled=True),
        lax.all_gather(gain_attn, "fsdp", axis=0, tiled=True),
        lax.all_gather(shift_attn, "fsdp", axis=0, tiled=True),
    )
    gain_one = gain_one.astype(jnp.float32)
    h_one = (unit_one * gain_one + shift_one.astype(jnp.float32)).astype(jnp.bfloat16)
    query = jnp.dot(h_one, wq_full, preferred_element_type=jnp.float32).astype(jnp.bfloat16)
    keys = jnp.dot(h_one, wk_full, preferred_element_type=jnp.float32).astype(jnp.bfloat16)
    fresh = jnp.dot(h_one, wv_full, preferred_element_type=jnp.float32).astype(jnp.bfloat16)
    fresh_heads = fresh.reshape(rows, seqs, local_heads // 2, HEAD_DIM)
    reused_heads = first_values.reshape(rows, seqs, local_heads // 2, HEAD_DIM)
    values = jnp.stack([fresh_heads, reused_heads], axis=3).reshape(rows, seqs, head_cols)
    keys_sent = keys.reshape(rows, seqs, head_cols)
    query4 = query.reshape(rows, seqs, local_heads, HEAD_DIM)
    absorb = make_absorb(query4, q_places, places_all, scale)
    start_state = (
        jnp.full((seqs, local_heads, rows), big_negative, jnp.float32),
        jnp.zeros((seqs, local_heads, rows), jnp.float32),
        jnp.zeros((rows, seqs, local_heads, HEAD_DIM), jnp.float32),
    )
    top, total, summed = absorb(
        start_state,
        (
            lax.all_gather(keys_sent, "ctx", axis=0, tiled=True),
            lax.all_gather(values, "ctx", axis=0, tiled=True),
        ),
        jnp.int32(0),
    )
    mixed_exact = summed / jnp.transpose(total, (2, 0, 1))[..., None]
    log_total = top + jnp.log(total)
    mixed = mixed_exact.reshape(count, head_cols).astype(jnp.bfloat16)
    resid = x_rows + lax.psum(contract_cols(mixed, wo_full).astype(jnp.bfloat16), "tp").astype(
        jnp.float32
    )
    unit_two, inverse_two = normalize_rows(resid)
    wu_full, wd_full, gain_two, shift_two = (
        lax.all_gather(w_up, "fsdp", axis=0, tiled=True),
        lax.all_gather(w_down, "fsdp", axis=0, tiled=True),
        lax.all_gather(gain_mlp, "fsdp", axis=0, tiled=True),
        lax.all_gather(shift_mlp, "fsdp", axis=0, tiled=True),
    )
    gain_two = gain_two.astype(jnp.float32)
    h_two = (unit_two * gain_two + shift_two.astype(jnp.float32)).astype(jnp.bfloat16)
    upper = jnp.dot(h_two, wu_full, preferred_element_type=jnp.float32)
    act = gelu_forward(upper).astype(jnp.bfloat16)
    out_rows = resid + lax.psum(contract_cols(act, wd_full).astype(jnp.bfloat16), "tp").astype(
        jnp.float32
    )
    d_out = cotangent.reshape(count, width)
    grad_down = contract_rows(d_out, act)
    d_act = jnp.dot(d_out, wd_full, preferred_element_type=jnp.float32)
    d_upper = (d_act * gelu_slope(upper)).astype(jnp.bfloat16)
    grad_up = contract_rows(h_two, d_upper)
    d_two = lax.psum(contract_cols(d_upper, wu_full).astype(jnp.bfloat16), "tp").astype(jnp.float32)
    grad_gain_mlp = jnp.sum(d_two * unit_two, axis=0)
    grad_shift_mlp = jnp.sum(d_two, axis=0)
    d_resid = d_out.astype(jnp.float32) + normalize_back(d_two, unit_two, inverse_two, gain_two)
    d_branch = d_resid.astype(jnp.bfloat16)
    grad_outproj = contract_rows(d_branch, mixed)
    d_mixed = jnp.dot(d_branch, wo_full, preferred_element_type=jnp.float32).astype(jnp.bfloat16)
    d_mixed4 = d_mixed.reshape(rows, seqs, local_heads, HEAD_DIM)
    delta = jnp.transpose(jnp.sum(d_mixed4.astype(jnp.float32) * mixed_exact, axis=-1), (1, 2, 0))
    zero_query = jnp.zeros((rows, seqs, local_heads, HEAD_DIM), jnp.float32)
    zero_keys = jnp.zeros((rows, seqs, head_cols), jnp.float32)

    def visit(step, state):
        moving_k, moving_v, acc_k, acc_v, acc_q = state
        source = (rank - step) % ranks
        p_block = lax.dynamic_slice_in_dim(places_all, source * rows, rows)
        part_q, part_k, part_v = grad_pair(
            query4,
            d_mixed4,
            delta,
            log_total,
            q_places,
            moving_k.reshape(rows, seqs, local_heads, HEAD_DIM),
            moving_v.reshape(rows, seqs, local_heads, HEAD_DIM),
            p_block,
            scale,
        )
        acc_k = acc_k + part_k.reshape(rows, seqs, head_cols)
        acc_v = acc_v + part_v.reshape(rows, seqs, head_cols)
        moving_k, moving_v = passed_along((moving_k, moving_v), "ctx", 1)
        acc_k, acc_v = (
            passed_along(acc_k.astype(jnp.bfloat16), "ctx", 1).astype(acc_k.dtype),
            passed_along(acc_v.astype(jnp.bfloat16), "ctx", 1).astype(acc_v.dtype),
        )
        return (moving_k, moving_v, acc_k, acc_v, acc_q + part_q)

    final_state = lax.fori_loop(
        0, ranks, visit, (keys_sent, values, zero_keys, zero_keys, zero_query)
    )
    d_keys = final_state[2]
    d_values = final_state[3]
    d_query = final_state[4]
    d_query_low = (d_query * scale).reshape(count, head_cols).astype(jnp.bfloat16)
    d_keys_low = (d_keys * scale).reshape(count, head_cols).astype(jnp.bfloat16)
    split_values = d_values.reshape(rows, seqs, local_heads // 2, 2, HEAD_DIM)
    d_fresh = split_values[:, :, :, 0, :].reshape(count, head_cols // 2).astype(jnp.bfloat16)
    grad_first = split_values[:, :, :, 1, :].reshape(rows, seqs, head_cols // 2)
    grad_query = contract_rows(h_one, d_query_low)
    grad_key = contract_rows(h_one, d_keys_low)
    grad_value = contract_rows(h_one, d_fresh)
    d_part = (
        contract_cols(d_query_low, wq_full)
        + contract_cols(d_keys_low, wk_full)
        + contract_cols(d_fresh, wv_full)
    )
    d_one = lax.psum(d_part.astype(jnp.bfloat16), "tp").astype(jnp.float32)
    grad_gain_attn = jnp.sum(d_one * unit_one, axis=0)
    grad_shift_attn = jnp.sum(d_one, axis=0)
    d_input = d_resid + normalize_back(d_one, unit_one, inverse_one, gain_one)
    shared = (
        lax.psum_scatter(
            grad_query.astype(jnp.bfloat16), "fsdp", scatter_dimension=0, tiled=True
        ).astype(jnp.float32),
        lax.psum_scatter(
            grad_key.astype(jnp.bfloat16), "fsdp", scatter_dimension=0, tiled=True
        ).astype(jnp.float32),
        lax.psum_scatter(
            grad_value.astype(jnp.bfloat16), "fsdp", scatter_dimension=0, tiled=True
        ).astype(jnp.float32),
        lax.psum_scatter(
            grad_outproj.astype(jnp.bfloat16), "fsdp", scatter_dimension=0, tiled=True
        ).astype(jnp.float32),
        lax.psum_scatter(
            grad_up.astype(jnp.bfloat16), "fsdp", scatter_dimension=0, tiled=True
        ).astype(jnp.float32),
        lax.psum_scatter(
            grad_down.astype(jnp.bfloat16), "fsdp", scatter_dimension=0, tiled=True
        ).astype(jnp.float32),
        lax.psum_scatter(
            grad_gain_attn.astype(jnp.bfloat16), "fsdp", scatter_dimension=0, tiled=True
        ).astype(jnp.float32),
        lax.psum_scatter(
            grad_shift_attn.astype(jnp.bfloat16), "fsdp", scatter_dimension=0, tiled=True
        ).astype(jnp.float32),
        lax.psum_scatter(
            grad_gain_mlp.astype(jnp.bfloat16), "fsdp", scatter_dimension=0, tiled=True
        ).astype(jnp.float32),
        lax.psum_scatter(
            grad_shift_mlp.astype(jnp.bfloat16), "fsdp", scatter_dimension=0, tiled=True
        ).astype(jnp.float32),
    )
    summed_grads = (
        lax.psum(shared[0].astype(jnp.bfloat16), "ctx").astype(jnp.float32),
        lax.psum(shared[1].astype(jnp.bfloat16), "ctx").astype(jnp.float32),
        lax.psum(shared[2].astype(jnp.bfloat16), "ctx").astype(jnp.float32),
        lax.psum(shared[3].astype(jnp.bfloat16), "ctx").astype(jnp.float32),
        lax.psum(shared[4].astype(jnp.bfloat16), "ctx").astype(jnp.float32),
        lax.psum(shared[5].astype(jnp.bfloat16), "ctx").astype(jnp.float32),
        lax.psum(shared[6].astype(jnp.bfloat16), "ctx").astype(jnp.float32),
        lax.psum(shared[7].astype(jnp.bfloat16), "ctx").astype(jnp.float32),
        lax.psum(shared[8].astype(jnp.bfloat16), "ctx").astype(jnp.float32),
        lax.psum(shared[9].astype(jnp.bfloat16), "ctx").astype(jnp.float32),
    )
    return (
        out_rows.reshape(rows, seqs, width),
        d_input.reshape(rows, seqs, width),
        grad_first,
        summed_grads[0],
        summed_grads[1],
        summed_grads[2],
        summed_grads[3],
        summed_grads[4],
        summed_grads[5],
        summed_grads[6],
        summed_grads[7],
        summed_grads[8],
        summed_grads[9],
    )


def swap_fsdp(value, flip):
    count = lax.axis_size("fsdp")
    return lax.ppermute(value, "fsdp", [(i, i ^ flip) for i in range(count)])


def swap_tp(value):
    return lax.ppermute(value, "tp", [(0, 1), (1, 0)])


def swap_ctx(value):
    return lax.ppermute(value, "ctx", [(0, 1), (1, 0)])


def gather_rows(shard):
    count = lax.axis_size("fsdp")
    me = lax.axis_index("fsdp")
    own = [(0, shard)] + [(2 * k, swap_fsdp(shard, 2 * k)) for k in range(1, count // 2)]
    blocks = own + [(flip | 1, swap_fsdp(block, 1)) for flip, block in own]
    whole = jnp.zeros((count,) + shard.shape, shard.dtype)
    for flip, block in blocks:
        whole = lax.dynamic_update_slice(whole, block[None], (me ^ flip, 0, 0))
    return whole.reshape(count * shard.shape[0], shard.shape[1])


def scatter_rows(grad):
    count = lax.axis_size("fsdp")
    me = lax.axis_index("fsdp")
    inner, outer = me & 1, me >> 1
    rows = grad.shape[0] // count
    parts = grad.astype(low).reshape(count // 2, 2, rows, grad.shape[1])
    keep = lax.dynamic_index_in_dim(parts, inner, 1, keepdims=False)
    send = lax.dynamic_index_in_dim(parts, inner ^ 1, 1, keepdims=False)
    pair = (keep.astype(wide) + swap_fsdp(send, 1).astype(wide)).astype(low)
    total = lax.dynamic_index_in_dim(pair, outer, 0, keepdims=False).astype(wide)
    for k in range(1, count // 2):
        piece = lax.dynamic_index_in_dim(pair, outer ^ k, 0, keepdims=False)
        total = total + swap_fsdp(piece, 2 * k).astype(wide)
    return total


def share_quarters(block):
    side = lax.axis_index("tp")
    halves = block.reshape(2, block.shape[0] // 2, block.shape[1])
    own = lax.dynamic_index_in_dim(halves, side, 0, keepdims=False)
    beside = lax.dynamic_index_in_dim(halves, 1 - side, 0, keepdims=False)
    across = swap_ctx(own)
    return jnp.stack([own, beside, across, swap_tp(across)])


def spread_quarter(own):
    pair = jnp.stack([own, swap_ctx(own)])
    other = swap_tp(pair)
    return jnp.stack([pair[0], other[0], pair[1], other[1]])


def sum_quarter(part):
    part = part.astype(low)
    mine = jnp.stack([part[0], part[2]]).astype(wide) + swap_tp(jnp.stack([part[1], part[3]])).astype(wide)
    return mine[0] + swap_ctx(mine[1].astype(low)).astype(wide)


def rows_back(own, beside):
    side = lax.axis_index("tp")
    return jnp.concatenate([jnp.where(side == 0, own, beside), jnp.where(side == 0, beside, own)], axis=0)


def heads_of(block, parity):
    split = block.reshape(block.shape[0], -1, 2, HEAD_DIM)
    return lax.dynamic_index_in_dim(split, parity, 2, keepdims=False).reshape(block.shape[0], -1)


def heads_join(own, other, rank):
    shape = (own.shape[0], -1, HEAD_DIM)
    even = jnp.where(rank == 0, own, other).reshape(shape)
    odd = jnp.where(rank == 0, other, own).reshape(shape)
    return jnp.stack([even, odd], axis=2).reshape(own.shape[0], -1)


def local_split(
    hidden_in,
    first_values,
    span_table,
    w_query,
    w_key,
    w_value,
    w_out,
    w_up,
    w_down,
    gain_attn,
    shift_attn,
    gain_mlp,
    shift_mlp,
    cotangent,
):
    rows, seqs, width = hidden_in.shape
    span = rows // 2
    count = 4 * span
    rank, side = lax.axis_index("ctx"), lax.axis_index("tp")
    shard_rows = w_query.shape[0]
    cols = w_query.shape[1] // 2
    heads = cols // HEAD_DIM
    units = w_up.shape[1] // 2
    scale = HEAD_DIM ** (-0.5)

    span_order = [span_table[rank ^ dc, side ^ dt] for dc in range(2) for dt in range(2)]
    places = jnp.concatenate([place * span + jnp.arange(span, dtype=jnp.int32) for place in span_order])

    gains = jnp.stack([gain_attn, shift_attn, gain_mlp, shift_mlp], axis=1)
    attn_shard = jnp.concatenate([heads_of(w_query, rank), heads_of(w_key, rank), w_value, gains], axis=1)
    late_shard = jnp.concatenate(
        [
            lax.dynamic_slice_in_dim(w_up, rank * units, units, 1),
            lax.dynamic_slice_in_dim(w_down, rank * units, units, 1),
            heads_of(w_out, rank),
            heads_of(w_out, 1 - rank),
        ],
        axis=1,
    )
    x_all = share_quarters(hidden_in.reshape(rows, width))
    attn_full = gather_rows(attn_shard)
    first = first_values.reshape(2, span, cols)
    first_far = lax.ppermute(first_values.reshape(rows, cols), "ctx", [(0, 1)]).reshape(2, span, cols)
    first_all = jnp.concatenate(
        [
            lax.dynamic_index_in_dim(first, side, 0, keepdims=False),
            lax.dynamic_index_in_dim(first, 1 - side, 0, keepdims=False),
            lax.dynamic_index_in_dim(first_far, side, 0, keepdims=False),
            lax.dynamic_index_in_dim(first_far, 1 - side, 0, keepdims=False),
        ],
        axis=0,
    )
    late_full = gather_rows(late_shard)
    cot_all = share_quarters(cotangent.reshape(rows, width))

    w_qkv = attn_full[:, : 3 * cols]
    gains_full = attn_full[:, 3 * cols :].astype(wide).T
    gain_one, shift_one, gain_two, shift_two = (gains_full[i] for i in range(4))
    wu_full, wd_full = late_full[:, :units], late_full[:, units : 2 * units]
    wo_half = late_full[:, 2 * units :]
    wo_own = wo_half[:, :cols]
    wo_full = jnp.concatenate([wo_half, swap_tp(wo_half)], axis=1)

    x_rows = x_all.reshape(count, width).astype(wide)
    unit_one, inverse_one = normalize_rows(x_rows)
    h_one = (unit_one * gain_one + shift_one).astype(low)
    qkv = jnp.dot(h_one, w_qkv, preferred_element_type=wide).astype(low)
    query = qkv[:, :cols].reshape(count, heads, HEAD_DIM)
    keys = qkv[:, cols : 2 * cols].reshape(count, heads, HEAD_DIM)
    values = jnp.where(rank == 0, qkv[:, 2 * cols :], first_all).reshape(count, heads, HEAD_DIM)

    allowed = (places[None, :] <= places[:, None])[None]
    scores = jnp.einsum("qhe,khe->hqk", query, keys, preferred_element_type=wide) * scale
    scores = jnp.where(allowed, scores, big_negative)
    top = jnp.max(scores, axis=-1, keepdims=True)
    weights = jnp.where(allowed, jnp.exp(scores - top), 0.0)
    weights = weights / jnp.sum(weights, axis=-1, keepdims=True)
    probs = weights.astype(low)
    mixed_exact = jnp.einsum("hqk,khe->qhe", probs, values, preferred_element_type=wide)
    mixed = mixed_exact.reshape(count, cols).astype(low)

    mixed_far = swap_ctx(mixed).reshape(2, 2, span, cols)[::-1].reshape(count, cols)
    mixed_chip = jnp.concatenate([mixed, mixed_far], axis=1)
    mixed_side = swap_tp(mixed_chip).reshape(2, 2, span, 2 * cols)[:, ::-1].reshape(count, 2 * cols)
    mixed_all = jnp.concatenate([mixed_chip, mixed_side], axis=1)
    resid = x_rows + contract_cols(mixed_all, wo_full)
    unit_two, inverse_two = normalize_rows(resid)
    h_two = (unit_two * gain_two + shift_two).astype(low)
    upper = jnp.dot(h_two, wu_full, preferred_element_type=wide)
    act = gelu_forward(upper).astype(low)
    cot_rows = cot_all.reshape(count, width)
    d_act = jnp.dot(cot_rows, wd_full, preferred_element_type=wide)
    d_upper = (d_act * gelu_slope(upper)).astype(low)
    d_two = sum_quarter(contract_cols(d_upper, wu_full).reshape(4, span, width))
    grad_down = scatter_rows(contract_rows(cot_rows, act))
    grad_up = scatter_rows(contract_rows(h_two, d_upper))
    out_sum = sum_quarter(contract_cols(act, wd_full).reshape(4, span, width)).astype(low)
    out_beside = swap_tp(out_sum)
    out_rows = rows_back(resid[:span] + out_sum.astype(wide), resid[span : 2 * span] + out_beside.astype(wide))

    unit_mine = unit_two[:span]
    d_resid = cot_rows[:span].astype(wide) + normalize_back(d_two, unit_mine, inverse_two[:span], gain_two)
    branch_all = spread_quarter(d_resid.astype(low)).reshape(count, width)
    grad_outproj = scatter_rows(contract_rows(branch_all, mixed))
    d_mixed = jnp.dot(branch_all, wo_own, preferred_element_type=wide).astype(low).reshape(count, heads, HEAD_DIM)
    delta = jnp.sum(d_mixed.astype(wide) * mixed_exact, axis=-1).T
    d_weights = jnp.einsum("qhe,khe->hqk", d_mixed, values, preferred_element_type=wide)
    d_scores = (weights * (d_weights - delta[..., None])).astype(low)
    d_query = jnp.einsum("hqk,khe->qhe", d_scores, keys, preferred_element_type=wide) * scale
    d_keys = jnp.einsum("hqk,qhe->khe", d_scores, query, preferred_element_type=wide) * scale
    d_values = jnp.einsum("hqk,qhe->khe", probs, d_mixed, preferred_element_type=wide).reshape(count, cols)
    d_fresh = jnp.where(rank == 0, d_values, 0.0)
    d_qkv = jnp.concatenate(
        [d_query.reshape(count, cols), d_keys.reshape(count, cols), d_fresh], axis=1
    ).astype(low)
    d_one_part = contract_cols(d_qkv, w_qkv)
    d_one = sum_quarter(d_one_part.reshape(4, span, width))
    grad_gains = jnp.stack(
        [
            jnp.sum(d_one_part * unit_one, axis=0),
            jnp.sum(d_one_part, axis=0),
            jnp.sum(d_two * unit_mine, axis=0),
            jnp.sum(d_two, axis=0),
        ],
        axis=1,
    )
    grad_last = scatter_rows(jnp.concatenate([contract_rows(h_one, d_qkv), grad_gains], axis=1))
    d_input = d_resid + normalize_back(d_one, unit_one[:span], inverse_one[:span], gain_one)
    d_input = rows_back(d_input, swap_tp(d_input.astype(low)).astype(wide))

    first_rows = rows_back(d_values[:span], d_values[span : 2 * span])
    first_sent = rows_back(d_values[2 * span : 3 * span], d_values[3 * span :]).astype(low)
    grad_first = jnp.where(rank == 0, lax.ppermute(first_sent, "ctx", [(1, 0)]).astype(wide), first_rows)

    ffn = jnp.concatenate([grad_up, grad_down], axis=1).astype(low)
    ffn_far = swap_ctx(ffn).astype(wide)
    ffn = ffn.astype(wide)
    first_ffn, second_ffn = jnp.where(rank == 0, ffn, ffn_far), jnp.where(rank == 0, ffn_far, ffn)
    grad_up = jnp.concatenate([first_ffn[:, :units], second_ffn[:, :units]], axis=1)
    grad_down = jnp.concatenate([first_ffn[:, units:], second_ffn[:, units:]], axis=1)
    last = jnp.concatenate([grad_last, grad_outproj], axis=1).astype(low)
    last_far = swap_ctx(last).astype(wide)
    last = last.astype(wide)
    gain_cols = slice(3 * cols, 3 * cols + 4)
    gain_sum = last[:, gain_cols] + last_far[:, gain_cols]
    gain_sum = gain_sum + swap_tp(gain_sum.astype(low)).astype(wide)
    out_cols = slice(3 * cols + 4, None)
    return (
        out_rows.reshape(rows, seqs, width),
        d_input.reshape(rows, seqs, width),
        grad_first.reshape(rows, seqs, cols),
        heads_join(last[:, :cols], last_far[:, :cols], rank),
        heads_join(last[:, cols : 2 * cols], last_far[:, cols : 2 * cols], rank),
        jnp.where(rank == 0, last, last_far)[:, 2 * cols : 3 * cols],
        heads_join(last[:, out_cols], last_far[:, out_cols], rank),
        grad_up,
        grad_down,
        gain_sum[:, 0],
        gain_sum[:, 1],
        gain_sum[:, 2],
        gain_sum[:, 3],
    )


def solution(mesh):
    local = local_split if mesh.shape["ctx"] == 2 and mesh.shape["tp"] == 2 else local_ring
    rows, heads, wide_rows = P("ctx", "fsdp", None), P("ctx", "fsdp", "tp"), P("fsdp", "tp")
    return jax.shard_map(
        local,
        mesh=mesh,
        in_specs=(rows, heads, P()) + (wide_rows,) * 6 + (P("fsdp"),) * 4 + (rows,),
        out_specs=(rows, rows, heads) + (wide_rows,) * 6 + (P("fsdp"),) * 4,
        check_vma=False,
    )
```

```python
import jax
import jax.numpy as jnp
from jax import lax
from jax.experimental import pallas as pl
from jax.experimental.pallas import tpu as pltpu
from jax.sharding import PartitionSpec as P

HEADS = 12
HEAD_DIM = 64
low = jnp.bfloat16
wide = jnp.float32


eps_norm = 1e-05
big_negative = -1e30
gelu_coef = 0.7978845608028654
cube_coef = 0.044715


def passed_along(value, axis, steps):
    count = lax.axis_size(axis)
    pairs = [(source, (source + steps) % count) for source in range(count)]
    return lax.ppermute(value, axis, pairs)


def normalize_rows(values):
    mean = jnp.mean(values, axis=-1, keepdims=True)
    centred = values - mean
    inverse = lax.rsqrt(jnp.mean(centred * centred, axis=-1, keepdims=True) + eps_norm)
    return (centred * inverse, inverse)


def normalize_back(d_norm, unit, inverse, gain):
    scaled = d_norm * gain
    inner = (
        scaled
        - jnp.mean(scaled, axis=-1, keepdims=True)
        - unit * jnp.mean(scaled * unit, axis=-1, keepdims=True)
    )
    return inverse * inner


def gelu_forward(values):
    return (
        0.5 * values * (1.0 + jnp.tanh(gelu_coef * (values + cube_coef * values * values * values)))
    )


def gelu_slope(values):
    tanh_val = jnp.tanh(gelu_coef * (values + cube_coef * values * values * values))
    return 0.5 * (1.0 + tanh_val) + 0.5 * values * (1.0 - tanh_val * tanh_val) * gelu_coef * (
        1.0 + 3.0 * cube_coef * values * values
    )


def contract_rows(left, right):
    return lax.dot_general(
        left, right, (((0,), (0,)), ((), ())), preferred_element_type=jnp.float32
    )


def contract_cols(left, right):
    return lax.dot_general(
        left, right, (((1,), (1,)), ((), ())), preferred_element_type=jnp.float32
    )


def block_scores(query, keys, q_places, k_places, scale):
    scores = jnp.einsum("qshe,kshe->shqk", query, keys, preferred_element_type=jnp.float32) * scale
    allowed = k_places[None, None, None, :] <= q_places[None, None, :, None]
    return (jnp.where(allowed, scores, big_negative), allowed)


def absorb_block(state, query, q_places, k_block, v_block, p_block, scale):
    top, total, summed = state
    scores, allowed = block_scores(query, k_block, q_places, p_block, scale)
    new_top = jnp.maximum(top, jnp.max(scores, axis=-1))
    factor = jnp.exp(top - new_top)
    weights = jnp.where(allowed, jnp.exp(scores - new_top[..., None]), 0.0)
    total = total * factor + jnp.sum(weights, axis=-1)
    update = jnp.einsum(
        "shqk,kshe->qshe", weights.astype(jnp.bfloat16), v_block, preferred_element_type=jnp.float32
    )
    summed = summed * jnp.transpose(factor, (2, 0, 1))[..., None] + update
    return (new_top, total, summed)


def make_absorb(query, q_places, places_all, scale):
    rows, seqs, heads, width = query.shape

    def absorb(carry, piece, start):
        keys, values = piece
        pairs = keys.shape[0] // rows
        k_pairs = keys.reshape(pairs, rows, seqs, heads, width)
        v_pairs = values.reshape(pairs, rows, seqs, heads, width)
        p_pairs = places_all.reshape(pairs, rows)

        def one_pair(state, item):
            k_pair, v_pair, p_pair = item
            return (absorb_block(state, query, q_places, k_pair, v_pair, p_pair, scale), None)

        carry, _ = lax.scan(one_pair, carry, (k_pairs, v_pairs, p_pairs))
        return carry

    return absorb


def grad_block(query, d_mixed, delta, log_total, q_places, k_block, v_block, p_block, scale):
    scores, allowed = block_scores(query, k_block, q_places, p_block, scale)
    weights = jnp.where(allowed, jnp.exp(scores - log_total[..., None]), 0.0)
    d_weights = jnp.einsum("qshe,kshe->shqk", d_mixed, v_block, preferred_element_type=jnp.float32)
    d_scores = (weights * (d_weights - delta[..., None])).astype(jnp.bfloat16)
    part_query = jnp.einsum(
        "shqk,kshe->qshe", d_scores, k_block, preferred_element_type=jnp.float32
    )
    part_key = jnp.einsum("shqk,qshe->kshe", d_scores, query, preferred_element_type=jnp.float32)
    part_value = jnp.einsum(
        "shqk,qshe->kshe", weights.astype(jnp.bfloat16), d_mixed, preferred_element_type=jnp.float32
    )
    return (part_query, part_key, part_value)


def grad_pair(query, d_mixed, delta, log_total, q_places, k_shard, v_shard, p_shard, scale):
    return grad_block(query, d_mixed, delta, log_total, q_places, k_shard, v_shard, p_shard, scale)


def local_ring(
    hidden_in,
    first_values,
    span_table,
    w_query,
    w_key,
    w_value,
    w_out,
    w_up,
    w_down,
    gain_attn,
    shift_attn,
    gain_mlp,
    shift_mlp,
    cotangent,
):
    rows, seqs, width = hidden_in.shape
    count = rows * seqs
    ranks = lax.axis_size("ctx")
    rank = lax.axis_index("ctx")
    span_rows = rows // 2
    local_heads = HEADS // lax.axis_size("tp")
    head_cols = local_heads * HEAD_DIM
    scale = HEAD_DIM ** (-0.5)
    places_all = (
        jnp.repeat(span_table.reshape(-1), span_rows) * span_rows
        + jnp.arange(ranks * rows, dtype=jnp.int32) % span_rows
    )
    q_places = lax.dynamic_slice_in_dim(places_all, rank * rows, rows)
    x_rows = hidden_in.reshape(count, width).astype(jnp.float32)
    unit_one, inverse_one = normalize_rows(x_rows)
    wq_full, wk_full, wv_full, wo_full, gain_one, shift_one = (
        lax.all_gather(w_query, "fsdp", axis=0, tiled=True),
        lax.all_gather(w_key, "fsdp", axis=0, tiled=True),
        lax.all_gather(w_value, "fsdp", axis=0, tiled=True),
        lax.all_gather(w_out, "fsdp", axis=0, tiled=True),
        lax.all_gather(gain_attn, "fsdp", axis=0, tiled=True),
        lax.all_gather(shift_attn, "fsdp", axis=0, tiled=True),
    )
    gain_one = gain_one.astype(jnp.float32)
    h_one = (unit_one * gain_one + shift_one.astype(jnp.float32)).astype(jnp.bfloat16)
    query = jnp.dot(h_one, wq_full, preferred_element_type=jnp.float32).astype(jnp.bfloat16)
    keys = jnp.dot(h_one, wk_full, preferred_element_type=jnp.float32).astype(jnp.bfloat16)
    fresh = jnp.dot(h_one, wv_full, preferred_element_type=jnp.float32).astype(jnp.bfloat16)
    fresh_heads = fresh.reshape(rows, seqs, local_heads // 2, HEAD_DIM)
    reused_heads = first_values.reshape(rows, seqs, local_heads // 2, HEAD_DIM)
    values = jnp.stack([fresh_heads, reused_heads], axis=3).reshape(rows, seqs, head_cols)
    keys_sent = keys.reshape(rows, seqs, head_cols)
    query4 = query.reshape(rows, seqs, local_heads, HEAD_DIM)
    absorb = make_absorb(query4, q_places, places_all, scale)
    start_state = (
        jnp.full((seqs, local_heads, rows), big_negative, jnp.float32),
        jnp.zeros((seqs, local_heads, rows), jnp.float32),
        jnp.zeros((rows, seqs, local_heads, HEAD_DIM), jnp.float32),
    )
    top, total, summed = absorb(
        start_state,
        (
            lax.all_gather(keys_sent, "ctx", axis=0, tiled=True),
            lax.all_gather(values, "ctx", axis=0, tiled=True),
        ),
        jnp.int32(0),
    )
    mixed_exact = summed / jnp.transpose(total, (2, 0, 1))[..., None]
    log_total = top + jnp.log(total)
    mixed = mixed_exact.reshape(count, head_cols).astype(jnp.bfloat16)
    resid = x_rows + lax.psum(contract_cols(mixed, wo_full).astype(jnp.bfloat16), "tp").astype(
        jnp.float32
    )
    unit_two, inverse_two = normalize_rows(resid)
    wu_full, wd_full, gain_two, shift_two = (
        lax.all_gather(w_up, "fsdp", axis=0, tiled=True),
        lax.all_gather(w_down, "fsdp", axis=0, tiled=True),
        lax.all_gather(gain_mlp, "fsdp", axis=0, tiled=True),
        lax.all_gather(shift_mlp, "fsdp", axis=0, tiled=True),
    )
    gain_two = gain_two.astype(jnp.float32)
    h_two = (unit_two * gain_two + shift_two.astype(jnp.float32)).astype(jnp.bfloat16)
    upper = jnp.dot(h_two, wu_full, preferred_element_type=jnp.float32)
    act = gelu_forward(upper).astype(jnp.bfloat16)
    out_rows = resid + lax.psum(contract_cols(act, wd_full).astype(jnp.bfloat16), "tp").astype(
        jnp.float32
    )
    d_out = cotangent.reshape(count, width)
    grad_down = contract_rows(d_out, act)
    d_act = jnp.dot(d_out, wd_full, preferred_element_type=jnp.float32)
    d_upper = (d_act * gelu_slope(upper)).astype(jnp.bfloat16)
    grad_up = contract_rows(h_two, d_upper)
    d_two = lax.psum(contract_cols(d_upper, wu_full).astype(jnp.bfloat16), "tp").astype(jnp.float32)
    grad_gain_mlp = jnp.sum(d_two * unit_two, axis=0)
    grad_shift_mlp = jnp.sum(d_two, axis=0)
    d_resid = d_out.astype(jnp.float32) + normalize_back(d_two, unit_two, inverse_two, gain_two)
    d_branch = d_resid.astype(jnp.bfloat16)
    grad_outproj = contract_rows(d_branch, mixed)
    d_mixed = jnp.dot(d_branch, wo_full, preferred_element_type=jnp.float32).astype(jnp.bfloat16)
    d_mixed4 = d_mixed.reshape(rows, seqs, local_heads, HEAD_DIM)
    delta = jnp.transpose(jnp.sum(d_mixed4.astype(jnp.float32) * mixed_exact, axis=-1), (1, 2, 0))
    zero_query = jnp.zeros((rows, seqs, local_heads, HEAD_DIM), jnp.float32)
    zero_keys = jnp.zeros((rows, seqs, head_cols), jnp.float32)

    def visit(step, state):
        moving_k, moving_v, acc_k, acc_v, acc_q = state
        source = (rank - step) % ranks
        p_block = lax.dynamic_slice_in_dim(places_all, source * rows, rows)
        part_q, part_k, part_v = grad_pair(
            query4,
            d_mixed4,
            delta,
            log_total,
            q_places,
            moving_k.reshape(rows, seqs, local_heads, HEAD_DIM),
            moving_v.reshape(rows, seqs, local_heads, HEAD_DIM),
            p_block,
            scale,
        )
        acc_k = acc_k + part_k.reshape(rows, seqs, head_cols)
        acc_v = acc_v + part_v.reshape(rows, seqs, head_cols)
        moving_k, moving_v = passed_along((moving_k, moving_v), "ctx", 1)
        acc_k, acc_v = (
            passed_along(acc_k.astype(jnp.bfloat16), "ctx", 1).astype(acc_k.dtype),
            passed_along(acc_v.astype(jnp.bfloat16), "ctx", 1).astype(acc_v.dtype),
        )
        return (moving_k, moving_v, acc_k, acc_v, acc_q + part_q)

    final_state = lax.fori_loop(
        0, ranks, visit, (keys_sent, values, zero_keys, zero_keys, zero_query)
    )
    d_keys = final_state[2]
    d_values = final_state[3]
    d_query = final_state[4]
    d_query_low = (d_query * scale).reshape(count, head_cols).astype(jnp.bfloat16)
    d_keys_low = (d_keys * scale).reshape(count, head_cols).astype(jnp.bfloat16)
    split_values = d_values.reshape(rows, seqs, local_heads // 2, 2, HEAD_DIM)
    d_fresh = split_values[:, :, :, 0, :].reshape(count, head_cols // 2).astype(jnp.bfloat16)
    grad_first = split_values[:, :, :, 1, :].reshape(rows, seqs, head_cols // 2)
    grad_query = contract_rows(h_one, d_query_low)
    grad_key = contract_rows(h_one, d_keys_low)
    grad_value = contract_rows(h_one, d_fresh)
    d_part = (
        contract_cols(d_query_low, wq_full)
        + contract_cols(d_keys_low, wk_full)
        + contract_cols(d_fresh, wv_full)
    )
    d_one = lax.psum(d_part.astype(jnp.bfloat16), "tp").astype(jnp.float32)
    grad_gain_attn = jnp.sum(d_one * unit_one, axis=0)
    grad_shift_attn = jnp.sum(d_one, axis=0)
    d_input = d_resid + normalize_back(d_one, unit_one, inverse_one, gain_one)
    shared = (
        lax.psum_scatter(
            grad_query.astype(jnp.bfloat16), "fsdp", scatter_dimension=0, tiled=True
        ).astype(jnp.float32),
        lax.psum_scatter(
            grad_key.astype(jnp.bfloat16), "fsdp", scatter_dimension=0, tiled=True
        ).astype(jnp.float32),
        lax.psum_scatter(
            grad_value.astype(jnp.bfloat16), "fsdp", scatter_dimension=0, tiled=True
        ).astype(jnp.float32),
        lax.psum_scatter(
            grad_outproj.astype(jnp.bfloat16), "fsdp", scatter_dimension=0, tiled=True
        ).astype(jnp.float32),
        lax.psum_scatter(
            grad_up.astype(jnp.bfloat16), "fsdp", scatter_dimension=0, tiled=True
        ).astype(jnp.float32),
        lax.psum_scatter(
            grad_down.astype(jnp.bfloat16), "fsdp", scatter_dimension=0, tiled=True
        ).astype(jnp.float32),
        lax.psum_scatter(
            grad_gain_attn.astype(jnp.bfloat16), "fsdp", scatter_dimension=0, tiled=True
        ).astype(jnp.float32),
        lax.psum_scatter(
            grad_shift_attn.astype(jnp.bfloat16), "fsdp", scatter_dimension=0, tiled=True
        ).astype(jnp.float32),
        lax.psum_scatter(
            grad_gain_mlp.astype(jnp.bfloat16), "fsdp", scatter_dimension=0, tiled=True
        ).astype(jnp.float32),
        lax.psum_scatter(
            grad_shift_mlp.astype(jnp.bfloat16), "fsdp", scatter_dimension=0, tiled=True
        ).astype(jnp.float32),
    )
    summed_grads = (
        lax.psum(shared[0].astype(jnp.bfloat16), "ctx").astype(jnp.float32),
        lax.psum(shared[1].astype(jnp.bfloat16), "ctx").astype(jnp.float32),
        lax.psum(shared[2].astype(jnp.bfloat16), "ctx").astype(jnp.float32),
        lax.psum(shared[3].astype(jnp.bfloat16), "ctx").astype(jnp.float32),
        lax.psum(shared[4].astype(jnp.bfloat16), "ctx").astype(jnp.float32),
        lax.psum(shared[5].astype(jnp.bfloat16), "ctx").astype(jnp.float32),
        lax.psum(shared[6].astype(jnp.bfloat16), "ctx").astype(jnp.float32),
        lax.psum(shared[7].astype(jnp.bfloat16), "ctx").astype(jnp.float32),
        lax.psum(shared[8].astype(jnp.bfloat16), "ctx").astype(jnp.float32),
        lax.psum(shared[9].astype(jnp.bfloat16), "ctx").astype(jnp.float32),
    )
    return (
        out_rows.reshape(rows, seqs, width),
        d_input.reshape(rows, seqs, width),
        grad_first,
        summed_grads[0],
        summed_grads[1],
        summed_grads[2],
        summed_grads[3],
        summed_grads[4],
        summed_grads[5],
        summed_grads[6],
        summed_grads[7],
        summed_grads[8],
        summed_grads[9],
    )


def swap_fsdp(value, flip):
    count = lax.axis_size("fsdp")
    return lax.ppermute(value, "fsdp", [(i, i ^ flip) for i in range(count)])


def swap_tp(value):
    return lax.ppermute(value, "tp", [(0, 1), (1, 0)])


def swap_ctx(value):
    return lax.ppermute(value, "ctx", [(0, 1), (1, 0)])


def gather_blocks(shard):
    count = lax.axis_size("fsdp")
    blocks = {0: shard}
    for k in range(1, count // 2):
        blocks[2 * k] = swap_fsdp(shard, 2 * k)
    for k in range(count // 2):
        blocks[2 * k + 1] = swap_fsdp(blocks[2 * k], 1)
    return [blocks[m] for m in range(count)]


def matmul(left, right, left_dim, right_dim):
    return lax.dot_general(left, right, (((left_dim,), (right_dim,)), ((), ())), preferred_element_type=wide)


def shapes(*pairs):
    return tuple(jax.ShapeDtypeStruct(shape, dtype) for shape, dtype in pairs)


def parity_heads(block, odd):
    count = block.shape[1] // HEAD_DIM
    return jnp.concatenate([block[:, j * HEAD_DIM : (j + 1) * HEAD_DIM] for j in range(odd, count, 2)], axis=1)


def woven_heads(even, odd):
    count = even.shape[1] // HEAD_DIM
    parts = []
    for i in range(count):
        parts += [even[:, i * HEAD_DIM : (i + 1) * HEAD_DIM], odd[:, i * HEAD_DIM : (i + 1) * HEAD_DIM]]
    return jnp.concatenate(parts, axis=1)


def pack_attn_kernel(wq, wk, wv, g0, g1, g2, g3, out):
    rank = lax.axis_index("ctx")
    shard = wq.shape[0]

    def pick(ref):
        block = ref[...].astype(wide)
        return jnp.where(rank == 0, parity_heads(block, 0), parity_heads(block, 1))

    gains = jnp.concatenate([g[...].astype(wide) for g in (g0, g1, g2, g3)] + [jnp.zeros((4, shard), wide)], axis=0)
    gains = jnp.concatenate([gains, jnp.zeros((8, 128 - shard), wide)], axis=1).T[:shard]
    pad = jnp.zeros((shard, HEAD_DIM - 8), wide)
    out[...] = jnp.concatenate([pick(wq), pick(wk), wv[...].astype(wide), gains, pad], axis=1).astype(low)


def pack_late_kernel(wo, wu, wd, out_up, out_down):
    rank = lax.axis_index("ctx")
    cols, units = wo.shape[1], wu.shape[1] // 2
    block = wo[...].astype(wide)
    even, odd = parity_heads(block, 0), parity_heads(block, 1)
    own = jnp.where(rank == 0, even, odd)
    other = jnp.where(rank == 0, odd, even)
    out_up[:, :cols] = jnp.concatenate([own, other], axis=1).astype(low)
    out_up[:, cols:] = jnp.where(rank == 0, wu[:, :units], wu[:, units:])
    out_down[...] = jnp.where(rank == 0, wd[:, :units], wd[:, units:])


def place_blocks(blocks, store):
    me = lax.axis_index("fsdp")
    for m, block in enumerate(blocks):
        rows = block.shape[0]
        store(pl.ds(pl.multiple_of((me ^ m) * rows, 32), rows), block)


def row_norm(values):
    mean = jnp.mean(values, axis=-1, keepdims=True)
    centred = values - mean
    inverse = lax.rsqrt(jnp.mean(centred * centred, axis=-1, keepdims=True) + eps_norm)
    return centred * inverse, inverse


def quarter_of_place(table):
    rank, side = lax.axis_index("ctx"), lax.axis_index("tp")
    held = [table[rank ^ (q // 2), side ^ (q % 2)] for q in range(4)]
    return [sum(jnp.where(held[q] == p, q, 0) for q in range(4)) for p in range(4)]


def attn_kernel(table, hid, across, across2, b0, b1, b2, b3, b4, b5, b6, b7, first, first_far,
                x_out, h_out, w_out, gains_out, qkv_out, mix_out, low_out, lse_out, keys_scr):
    rank, side = lax.axis_index("ctx"), lax.axis_index("tp")
    span = across.shape[0]
    cols = first.shape[0]
    heads = cols // HEAD_DIM

    def store(where, block):
        w_out[where, :] = block[...]

    place_blocks((b0, b1, b2, b3, b4, b5, b6, b7), store)
    gains = w_out[:, 512:640].astype(wide).T[64:72]
    gains_out[...] = gains
    gain, shift = gains[0:1], gains[1:2]
    x_out[0] = hid[pl.ds(pl.multiple_of(side * span, span), span), :]
    x_out[1] = hid[pl.ds(pl.multiple_of((1 - side) * span, span), span), :]
    x_out[2] = across[...]
    x_out[3] = across2[...]
    step = 64

    def norm_chunk(i, carry):
        for q in range(4):
            where = pl.ds(pl.multiple_of(i * step, step), step)
            unit, _ = row_norm(x_out[q, where, :].astype(wide))
            h_out[q, where, :] = (unit * gain + shift).astype(low)
        return carry

    lax.fori_loop(0, span // step, norm_chunk, 0)
    w_turned = w_out[:, : 3 * cols].T
    for q in range(4):
        qkv_out[q] = matmul(w_turned, h_out[q], 1, 1).astype(low)

    @pl.when(rank == 1)
    def _():
        for q in range(4):
            ref = first if q < 2 else first_far
            half = side if q % 2 == 0 else 1 - side
            qkv_out[q, 2 * cols :, :] = jnp.where(half == 0, ref[:, :span], ref[:, span:])

    order = quarter_of_place(table)
    below = lax.broadcasted_iota(jnp.int32, (span, span), 0) <= lax.broadcasted_iota(jnp.int32, (span, span), 1)
    lse_out[...] = jnp.zeros_like(lse_out)

    for h in range(heads):
        base = h * HEAD_DIM
        for p in range(4):
            keys_scr[p] = qkv_out[order[p], cols + base : cols + base + HEAD_DIM, :].T
        for qp in range(4):
            query = qkv_out[order[qp], base : base + HEAD_DIM, :] * low(HEAD_DIM ** -0.5)
            scores = [matmul(keys_scr[kp], query, 1, 0) for kp in range(qp + 1)]
            scores[qp] = jnp.where(below, scores[qp], big_negative)
            top = jnp.max(scores[0], axis=0, keepdims=True)
            for s in scores[1:]:
                top = jnp.maximum(top, jnp.max(s, axis=0, keepdims=True))
            total = jnp.zeros((1, span), wide)
            mixed = jnp.zeros((HEAD_DIM, span), wide)
            for kp in range(qp + 1):
                weights = jnp.exp(scores[kp] - top)
                total = total + jnp.sum(weights, axis=0, keepdims=True)
                value = qkv_out[order[kp], 2 * cols + base : 2 * cols + base + HEAD_DIM, :]
                mixed = mixed + matmul(value, weights.astype(low), 1, 0)
            mixed = mixed / total
            mix_out[order[qp], base : base + HEAD_DIM, :] = mixed
            low_out[order[qp], base : base + HEAD_DIM, :] = mixed.astype(low)
            lse_out[order[qp], h : h + 1, :] = top + jnp.log(total)


def place_up_kernel(b0, b1, b2, b3, b4, b5, b6, b7, wo_out, wu_out):
    cols = wo_out.shape[1]

    def store(where, block):
        wo_out[where, :] = block[:, :cols]
        wu_out[where, :] = block[:, cols:]

    place_blocks((b0, b1, b2, b3, b4, b5, b6, b7), store)


def place_down_kernel(b0, b1, b2, b3, b4, b5, b6, b7, cot, across, across2, wd_out, cot_out):
    side = lax.axis_index("tp")
    span = across.shape[0]

    def store(where, block):
        wd_out[where, :] = block[...]

    place_blocks((b0, b1, b2, b3, b4, b5, b6, b7), store)
    cot_out[0] = cot[pl.ds(pl.multiple_of(side * span, span), span), :]
    cot_out[1] = cot[pl.ds(pl.multiple_of((1 - side) * span, span), span), :]
    cot_out[2] = across[...]
    cot_out[3] = across2[...]


def mlp_kernel(x, mix0, mix1, mix2, mix3, wo_own, wo_side, wu, wd, gains, cot,
               resid_out, act_out, h_out, dup_out, keep_out, send_out):
    q = pl.program_id(0)
    mixed = jnp.concatenate([mix0[0], mix1[0], mix2[0], mix3[0]], axis=0).T
    half = wo_own.shape[1]
    proj = matmul(mixed[:, :half], wo_own[...], 1, 1) + matmul(mixed[:, half:], wo_side[...], 1, 1)
    resid = x[0].astype(wide) + proj

    @pl.when(q < 2)
    def _():
        resid_out[0] = resid

    unit, _ = row_norm(resid)
    h_two = (unit * gains[2:3, :] + gains[3:4, :]).astype(low)
    h_out[0] = h_two
    upper = matmul(h_two, wu[...], 1, 0)
    square = upper * upper
    tanh = jnp.tanh(gelu_coef * upper * (1.0 + cube_coef * square))
    act_out[0] = (0.5 * upper * (1.0 + tanh)).astype(low)
    slope = 0.5 * (1.0 + tanh) + 0.5 * upper * (1.0 - tanh * tanh) * gelu_coef * (1.0 + 3.0 * cube_coef * square)
    d_act = matmul(cot[0], wd[...], 1, 0)
    d_upper = (d_act * slope).astype(low)
    dup_out[0] = d_upper
    part = matmul(d_upper, wu[...], 1, 1).astype(low)

    @pl.when(q % 2 == 0)
    def _():
        keep_out[0] = part

    @pl.when(q % 2 == 1)
    def _():
        send_out[0] = part


def scatter_slots(value, keep, send, lanes):
    me = lax.axis_index("fsdp")
    rows = keep.shape[1]
    for k in range(keep.shape[0]):
        base = (me >> 1) ^ k
        keep[k, :, lanes] = value[pl.ds(pl.multiple_of((base * 2 + (me & 1)) * rows, 32), rows), :].astype(low)
        send[k, :, lanes] = value[pl.ds(pl.multiple_of((base * 2 + ((me & 1) ^ 1)) * rows, 32), rows), :].astype(low)


def mlp_grad_kernel(cot, act, h_two, d_upper, wd, keep_out, send_out, out_keep, out_send, grad):
    units = act.shape[2]
    width = cot.shape[2]
    for left, right, first in ((h_two, d_upper, 0), (cot, act, units)):
        total = matmul(left[0], right[0], 0, 0)
        for q in range(1, 4):
            total = total + matmul(left[q], right[q], 0, 0)
        grad[...] = total
        scatter_slots(grad, keep_out, send_out, slice(first, first + units))
    for q in range(4):
        part = matmul(act[q], wd[...], 1, 1).astype(low)
        (out_keep if q % 2 == 0 else out_send)[q // 2] = part


def norm_back(d_norm, unit, inverse, gain):
    scaled = d_norm * gain
    inner = scaled - jnp.mean(scaled, axis=-1, keepdims=True) - unit * jnp.mean(scaled * unit, axis=-1, keepdims=True)
    return inverse * inner


def branch_kernel(keep, got, far, resid, cot, gains, d_resid_out, low_out, sums_out):
    d_two = keep[0].astype(wide) + got[0].astype(wide) + far[...].astype(wide)
    unit, inverse = row_norm(resid[0])
    sums_out[...] = jnp.zeros_like(sums_out)
    sums_out[0:1, :] = jnp.sum(d_two * unit, axis=0, keepdims=True)
    sums_out[1:2, :] = jnp.sum(d_two, axis=0, keepdims=True)
    d_resid = cot[0].astype(wide) + norm_back(d_two, unit, inverse, gains[2:3, :])
    d_resid_out[...] = d_resid
    low_out[...] = d_resid.astype(low)


def attn_back_kernel(table, br0, br1, br2, br3, wo, qkv, mix, lse, low_mix, d_out, d_first, keep_out, send_out,
                     dm_scr, keys_scr, values_scr, dq_scr, grad):
    rank = lax.axis_index("ctx")
    span = qkv.shape[2]
    cols = mix.shape[1]
    heads = cols // HEAD_DIM
    wo_turned = wo[:, :cols].T
    branches = (br0, br1, br2, br3)
    turned = jnp.zeros((cols, wo.shape[0]), wide)
    for q in range(4):
        dm_scr[q] = matmul(wo_turned, branches[q][...], 1, 1).astype(low)
        turned = turned + matmul(low_mix[q], branches[q][...], 1, 0)
    grad[...] = turned.T
    scatter_slots(grad, keep_out, send_out, slice(0, cols))
    order = quarter_of_place(table)
    below = lax.broadcasted_iota(jnp.int32, (span, span), 0) <= lax.broadcasted_iota(jnp.int32, (span, span), 1)
    root = low(HEAD_DIM ** -0.5)
    for h in range(heads):
        base = h * HEAD_DIM
        mine = slice(base, base + HEAD_DIM)
        delta = []
        for p in range(4):
            keys_scr[p] = qkv[order[p], cols + base : cols + base + HEAD_DIM, :].T
            values_scr[p] = qkv[order[p], 2 * cols + base : 2 * cols + base + HEAD_DIM, :].T
            delta.append(jnp.sum(dm_scr[order[p], mine, :].astype(wide) * mix[order[p], mine, :], axis=0, keepdims=True))
        for kp in range(4):
            d_key = jnp.zeros((HEAD_DIM, span), wide)
            d_value = jnp.zeros((HEAD_DIM, span), wide)
            key = qkv[order[kp], cols + base : cols + base + HEAD_DIM, :]
            for qp in range(kp, 4):
                query = qkv[order[qp], mine, :] * root
                d_mixed = dm_scr[order[qp], mine, :]
                weights = jnp.exp(matmul(keys_scr[kp], query, 1, 0) - lse[order[qp], h : h + 1, :])
                if kp == qp:
                    weights = jnp.where(below, weights, 0.0)
                d_weights = matmul(values_scr[kp], d_mixed, 1, 0)
                d_scores = (weights * (d_weights - delta[qp])).astype(low)
                d_value = d_value + matmul(d_mixed, weights.astype(low), 1, 1)
                d_key = d_key + matmul(query, d_scores, 1, 1)
                d_query = matmul(key, d_scores, 1, 0)
                dq_scr[qp] = d_query if kp == 0 else dq_scr[qp] + d_query
            d_out[order[kp], cols + base : cols + base + HEAD_DIM, :] = d_key.astype(low)
            d_first[order[kp], mine, :] = d_value
            d_out[order[kp], 2 * cols + base : 2 * cols + base + HEAD_DIM, :] = jnp.where(rank == 0, d_value, 0.0).astype(low)
        for qp in range(4):
            d_out[order[qp], mine, :] = (dq_scr[qp] * HEAD_DIM ** -0.5).astype(low)


def d_one_kernel(d_qkv, w, x, keep_out, send_out, sums_out):
    q = pl.program_id(0)
    wide_cols = d_qkv.shape[1]
    part = matmul(d_qkv[0].T, w[:, :wide_cols], 1, 1)
    unit, _ = row_norm(x[0].astype(wide))

    @pl.when(q == 0)
    def _():
        sums_out[...] = jnp.zeros_like(sums_out)

    sums_out[0:1, :] += jnp.sum(part * unit, axis=0, keepdims=True)
    sums_out[1:2, :] += jnp.sum(part, axis=0, keepdims=True)

    @pl.when(q % 2 == 0)
    def _():
        keep_out[0] = part.astype(low)

    @pl.when(q % 2 == 1)
    def _():
        send_out[0] = part.astype(low)


def attn_grad_kernel(d_qkv, h_one, sums_one, sums_two, side_one, side_two, keep_out, send_out, grad):
    cols = d_qkv.shape[1]
    width = h_one.shape[2]
    turned = matmul(d_qkv[0], h_one[0], 1, 0)
    for q in range(1, 4):
        turned = turned + matmul(d_qkv[q], h_one[q], 1, 0)
    grad[:, :cols] = turned.T
    one = sums_one[...] + side_one[...].astype(wide)
    two = sums_two[...] + side_two[...].astype(wide)
    sums = jnp.concatenate([one[0:2], two[0:2], jnp.zeros((124, width), wide)], axis=0).T
    grad[:, cols:] = sums[:, :HEAD_DIM]
    scatter_slots(grad, keep_out, send_out, slice(0, cols + HEAD_DIM))


def pair_kernel(keep, got, *outs):
    for k, out in enumerate(outs):
        out[...] = (keep[k].astype(wide) + got[k].astype(wide)).astype(low)


def total_kernel(a, b, c, d, out):
    out[...] = (a[...].astype(wide) + b[...].astype(wide) + c[...].astype(wide) + d[...].astype(wide)).astype(low)


def scatter_over(keep, send):
    shape = keep.shape[1:]
    parts = pl.pallas_call(pair_kernel, out_shape=shapes(*[(shape, low)] * keep.shape[0]))(keep, swap_fsdp(send, 1))
    found = [parts[0]] + [swap_fsdp(parts[k], 2 * k) for k in range(1, keep.shape[0])]
    return pl.pallas_call(total_kernel, out_shape=jax.ShapeDtypeStruct(shape, low))(*found)


def finish_mlp_kernel(own, far, up_out, down_out):
    rank = lax.axis_index("ctx")
    units = own.shape[1] // 2
    a, b = own[...].astype(wide), far[...].astype(wide)
    lower, upper = jnp.where(rank == 0, a, b), jnp.where(rank == 0, b, a)
    up_out[:, :units] = lower[:, :units]
    up_out[:, units:] = upper[:, :units]
    down_out[:, :units] = lower[:, units:]
    down_out[:, units:] = upper[:, units:]


def finish_attn_kernel(own, far, own_proj, far_proj, q_out, k_out, v_out, o_out, g0, g1, g2, g3):
    rank = lax.axis_index("ctx")
    cols = v_out.shape[1]
    rows = own.shape[0]
    a, b = own[...].astype(wide), far[...].astype(wide)
    even, odd = jnp.where(rank == 0, a, b), jnp.where(rank == 0, b, a)
    q_out[...] = woven_heads(even[:, :cols], odd[:, :cols])
    k_out[...] = woven_heads(even[:, cols : 2 * cols], odd[:, cols : 2 * cols])
    v_out[...] = even[:, 2 * cols : 3 * cols]
    c, d = own_proj[...].astype(wide), far_proj[...].astype(wide)
    o_out[...] = woven_heads(jnp.where(rank == 0, c, d), jnp.where(rank == 0, d, c))
    both = a[:, 512:640] + b[:, 512:640]
    gains = jnp.concatenate([both, jnp.zeros((128 - rows, 128), wide)], axis=0).T
    for i, out in enumerate((g0, g1, g2, g3)):
        out[...] = gains[64 + i : 65 + i, :rows]


def store_rows(out, first, value):
    pieces = value.shape[1] // 128
    for j in range(pieces):
        out[pl.ds(first * pieces + j, value.shape[0], stride=pieces), :] = value[:, j * 128 : (j + 1) * 128]


def out_kernel(resid, own, beside, out):
    side = lax.axis_index("tp")
    span = own.shape[0]
    store_rows(out, side * span, resid[0] + own[...].astype(wide))
    store_rows(out, (1 - side) * span, resid[1] + beside[...].astype(wide))


def input_grad_kernel(x, own, beside, d_own, d_beside, gains, out):
    side = lax.axis_index("tp")
    span = own.shape[0]
    for k, (d_one, d_resid) in enumerate(((own, d_own), (beside, d_beside))):
        unit, inverse = row_norm(x[k].astype(wide))
        value = d_resid[...] + norm_back(d_one[...].astype(wide), unit, inverse, gains[0:1, :])
        store_rows(out, (side if k == 0 else 1 - side) * span, value)


def first_grad_kernel(d_first, far, out):
    rank, side = lax.axis_index("ctx"), lax.axis_index("tp")
    span = d_first.shape[2]

    @pl.when(rank == 0)
    def _():
        out[...] = far[...].astype(wide)

    @pl.when(rank == 1)
    def _():
        out[:, :span] = jnp.where(side == 0, d_first[0], d_first[1])
        out[:, span:] = jnp.where(side == 0, d_first[1], d_first[0])


def first_send_kernel(d_first, out):
    side = lax.axis_index("tp")
    span = d_first.shape[2]
    out[:, :span] = jnp.where(side == 0, d_first[2], d_first[3]).astype(low)
    out[:, span:] = jnp.where(side == 0, d_first[3], d_first[2]).astype(low)


def sum_kernel(keep, got, out):
    out[...] = (keep[1].astype(wide) + got[1].astype(wide)).astype(low)


def close_kernel(keep, got, far, out):
    out[...] = (keep[0].astype(wide) + got[0].astype(wide) + far[...].astype(wide)).astype(low)


def local_split(
    hidden_in,
    first_values,
    span_table,
    w_query,
    w_key,
    w_value,
    w_out,
    w_up,
    w_down,
    gain_attn,
    shift_attn,
    gain_mlp,
    shift_mlp,
    cotangent,
):
    rows, seqs, width = hidden_in.shape
    span = rows // 2
    shard = w_query.shape[0]
    cols = w_query.shape[1] // 2
    units = w_up.shape[1] // 2
    pairs = lax.axis_size("fsdp") // 2
    smem = pl.BlockSpec(memory_space=pltpu.SMEM)
    vmem = pl.BlockSpec(memory_space=pltpu.VMEM)
    side = lax.axis_index("tp")

    def quarter_spec(c, turn=lambda q: q, s=span):
        return pl.BlockSpec((1, s, c), lambda q: (turn(q), 0, 0))

    def whole_spec(*shape):
        return pl.BlockSpec(shape, lambda q: (0,) * len(shape))

    def own_quarter(block):
        return lax.dynamic_slice_in_dim(block, side * span, span)

    hidden = hidden_in.reshape(rows, width)
    cot = cotangent.reshape(rows, width)
    first = first_values.reshape(rows, cols).T

    across = swap_ctx(own_quarter(hidden))
    gains_in = [g.reshape(1, shard) for g in (gain_attn, shift_attn, gain_mlp, shift_mlp)]
    attn_shard = pl.pallas_call(pack_attn_kernel, out_shape=jax.ShapeDtypeStruct((shard, 640), low))(
        w_query, w_key, w_value, *gains_in
    )
    attn_blocks = gather_blocks(attn_shard)
    across2 = swap_tp(across)
    first_far = lax.ppermute(first, "ctx", [(0, 1)])
    up_shard, down_shard = pl.pallas_call(
        pack_late_kernel, out_shape=shapes(((shard, 2 * cols + units), low), ((shard, units), low))
    )(w_out, w_up, w_down)
    up_blocks = gather_blocks(up_shard)
    cot_across = swap_ctx(own_quarter(cot))
    cot_across2 = swap_tp(cot_across)
    down_blocks = gather_blocks(down_shard)

    x4, h_one, w_qkv, gains, qkv, mix, low_mix, lse = pl.pallas_call(
        attn_kernel,
        in_specs=[smem] + [vmem] * 13,
        out_shape=shapes(
            ((4, span, width), low), ((4, span, width), low), ((width, 640), low), ((8, width), wide),
            ((4, 3 * cols, span), low), ((4, cols, span), wide), ((4, cols, span), low), ((4, 8, span), wide),
        ),
        scratch_shapes=[pltpu.VMEM((4, span, HEAD_DIM), low)],
    )(span_table, hidden, across, across2, *attn_blocks, first, first_far)

    mix_side = swap_tp(low_mix)
    mix_far = swap_ctx(low_mix)
    wo_half, wu = pl.pallas_call(place_up_kernel, out_shape=shapes(((width, 2 * cols), low), ((width, units), low)))(
        *up_blocks
    )
    wo_side = swap_tp(wo_half)
    mix_side_far = swap_tp(mix_far)
    wd, cot4 = pl.pallas_call(
        place_down_kernel, out_shape=shapes(((width, units), low), ((4, span, width), low))
    )(*down_blocks, cot, cot_across, cot_across2)

    half_spec = pl.BlockSpec((1, span, width), lambda q: (q // 2, 0, 0))
    resid, act, h_two, d_upper, two_keep, two_send = pl.pallas_call(
        mlp_kernel,
        grid=(4,),
        in_specs=[
            quarter_spec(width),
            quarter_spec(span, s=cols),
            quarter_spec(span, lambda q: (q + 2) % 4, cols),
            quarter_spec(span, lambda q: q + 1 - 2 * (q % 2), cols),
            quarter_spec(span, lambda q: 3 - q, cols),
            whole_spec(width, 2 * cols),
            whole_spec(width, 2 * cols),
            whole_spec(width, units),
            whole_spec(width, units),
            whole_spec(8, width),
            quarter_spec(width),
        ],
        out_specs=[
            quarter_spec(width, lambda q: jnp.minimum(q, 1)),
            quarter_spec(units),
            quarter_spec(width),
            quarter_spec(units),
            half_spec,
            half_spec,
        ],
        out_shape=shapes(
            ((2, span, width), wide), ((4, span, units), low), ((4, span, width), low), ((4, span, units), low),
            ((2, span, width), low), ((2, span, width), low),
        ),
    )(x4, low_mix, mix_far, mix_side, mix_side_far, wo_half, wo_side, wu, wd, gains, cot4)

    two_got = swap_tp(two_send)
    tile = jax.ShapeDtypeStruct((span, width), low)
    two_far = swap_ctx(pl.pallas_call(sum_kernel, out_shape=tile)(two_keep, two_got))
    mlp_keep, mlp_send, out_keep, out_send = pl.pallas_call(
        mlp_grad_kernel,
        out_shape=shapes(
            ((pairs, shard, 2 * units), low), ((pairs, shard, 2 * units), low), ((2, span, width), low), ((2, span, width), low)
        ),
        scratch_shapes=[pltpu.VMEM((width, units), wide)],
    )(cot4, act, h_two, d_upper, wd)
    d_resid, branch, sums_two = pl.pallas_call(
        branch_kernel,
        out_shape=shapes(((span, width), wide), ((span, width), low), ((8, width), wide)),
    )(two_keep, two_got, two_far, resid, cot4, gains)
    branch_far = swap_ctx(branch)
    branch_side = swap_tp(branch)
    d_resid_beside = swap_tp(d_resid)
    sums_two_side = swap_tp(sums_two.astype(low))
    branch_side_far = swap_tp(branch_far)
    mlp_total = scatter_over(mlp_keep, mlp_send)

    d_qkv, d_first, proj_keep, proj_send = pl.pallas_call(
        attn_back_kernel,
        in_specs=[smem] + [vmem] * 9,
        out_shape=shapes(
            ((4, 3 * cols, span), low), ((4, cols, span), wide), ((pairs, shard, cols), low), ((pairs, shard, cols), low)
        ),
        scratch_shapes=[
            pltpu.VMEM((4, cols, span), low),
            pltpu.VMEM((4, span, HEAD_DIM), low),
            pltpu.VMEM((4, span, HEAD_DIM), low),
            pltpu.VMEM((4, HEAD_DIM, span), wide),
            pltpu.VMEM((width, cols), wide),
        ],
    )(span_table, branch, branch_side, branch_far, branch_side_far, wo_half, qkv, mix, lse, low_mix)

    one_keep, one_send, sums_one = pl.pallas_call(
        d_one_kernel,
        grid=(4,),
        in_specs=[quarter_spec(span, s=3 * cols), whole_spec(width, 640), quarter_spec(width)],
        out_specs=[half_spec, half_spec, whole_spec(8, width)],
        out_shape=shapes(((2, span, width), low), ((2, span, width), low), ((8, width), wide)),
    )(d_qkv, w_qkv, x4)
    sums_one_side = swap_tp(sums_one.astype(low))
    one_got = swap_tp(one_send)
    one_far = swap_ctx(pl.pallas_call(sum_kernel, out_shape=tile)(one_keep, one_got))
    last_keep, last_send = pl.pallas_call(
        attn_grad_kernel,
        out_shape=shapes(((pairs, shard, 640), low), ((pairs, shard, 640), low)),
        scratch_shapes=[pltpu.VMEM((width, 640), wide)],
    )(d_qkv, h_one, sums_one, sums_two, sums_one_side, sums_two_side)
    proj_total = scatter_over(proj_keep, proj_send)
    last_total = scatter_over(last_keep, last_send)

    out_got = swap_tp(out_send)
    out_far = swap_ctx(pl.pallas_call(sum_kernel, out_shape=tile)(out_keep, out_got))
    out_sum = pl.pallas_call(close_kernel, out_shape=tile)(out_keep, out_got, out_far)
    flat = jax.ShapeDtypeStruct((rows * width // 128, 128), wide)
    out_rows = pl.pallas_call(out_kernel, out_shape=flat)(resid, out_sum, swap_tp(out_sum))

    one_sum = pl.pallas_call(close_kernel, out_shape=tile)(one_keep, one_got, one_far)
    d_input = pl.pallas_call(input_grad_kernel, out_shape=flat)(
        x4, one_sum, swap_tp(one_sum), d_resid, d_resid_beside, gains
    )

    first_sent = pl.pallas_call(first_send_kernel, out_shape=jax.ShapeDtypeStruct((cols, rows), low))(d_first)
    grad_first = pl.pallas_call(first_grad_kernel, out_shape=jax.ShapeDtypeStruct((cols, rows), wide))(
        d_first, lax.ppermute(first_sent, "ctx", [(1, 0)])
    )

    grad_up, grad_down = pl.pallas_call(finish_mlp_kernel, out_shape=shapes(*[((shard, 2 * units), wide)] * 2))(
        mlp_total, swap_ctx(mlp_total)
    )
    grads = pl.pallas_call(
        finish_attn_kernel,
        out_shape=shapes(
            ((shard, 2 * cols), wide), ((shard, 2 * cols), wide), ((shard, cols), wide), ((shard, 2 * cols), wide),
            *[((1, shard), wide)] * 4,
        ),
    )(last_total, swap_ctx(last_total), proj_total, swap_ctx(proj_total))
    return (
        out_rows.reshape(rows, seqs, width),
        d_input.reshape(rows, seqs, width),
        grad_first.T.reshape(rows, seqs, cols),
        grads[0],
        grads[1],
        grads[2],
        grads[3],
        grad_up,
        grad_down,
        *[g.reshape(shard) for g in grads[4:]],
    )


def solution(mesh):
    local = local_split if mesh.shape["ctx"] == 2 and mesh.shape["tp"] == 2 else local_ring
    rows, heads, wide_rows = P("ctx", "fsdp", None), P("ctx", "fsdp", "tp"), P("fsdp", "tp")
    return jax.shard_map(
        local,
        mesh=mesh,
        in_specs=(rows, heads, P()) + (wide_rows,) * 6 + (P("fsdp"),) * 4 + (rows,),
        out_specs=(rows, rows, heads) + (wide_rows,) * 6 + (P("fsdp"),) * 4,
        check_vma=False,
    )
```

```python
import jax
import jax.numpy as jnp
from jax import lax
from jax.experimental import pallas as pl
from jax.experimental.pallas import tpu as pltpu
from jax.sharding import PartitionSpec as P

HEADS = 12
HEAD_DIM = 64
low = jnp.bfloat16
wide = jnp.float32


eps_norm = 1e-05
big_negative = -1e30
gelu_coef = 0.7978845608028654
cube_coef = 0.044715


def passed_along(value, axis, steps):
    count = lax.axis_size(axis)
    pairs = [(source, (source + steps) % count) for source in range(count)]
    return lax.ppermute(value, axis, pairs)


def normalize_rows(values):
    mean = jnp.mean(values, axis=-1, keepdims=True)
    centred = values - mean
    inverse = lax.rsqrt(jnp.mean(centred * centred, axis=-1, keepdims=True) + eps_norm)
    return (centred * inverse, inverse)


def normalize_back(d_norm, unit, inverse, gain):
    scaled = d_norm * gain
    inner = (
        scaled
        - jnp.mean(scaled, axis=-1, keepdims=True)
        - unit * jnp.mean(scaled * unit, axis=-1, keepdims=True)
    )
    return inverse * inner


def gelu_forward(values):
    return (
        0.5 * values * (1.0 + jnp.tanh(gelu_coef * (values + cube_coef * values * values * values)))
    )


def gelu_slope(values):
    tanh_val = jnp.tanh(gelu_coef * (values + cube_coef * values * values * values))
    return 0.5 * (1.0 + tanh_val) + 0.5 * values * (1.0 - tanh_val * tanh_val) * gelu_coef * (
        1.0 + 3.0 * cube_coef * values * values
    )


def contract_rows(left, right):
    return lax.dot_general(
        left, right, (((0,), (0,)), ((), ())), preferred_element_type=jnp.float32
    )


def contract_cols(left, right):
    return lax.dot_general(
        left, right, (((1,), (1,)), ((), ())), preferred_element_type=jnp.float32
    )


def block_scores(query, keys, q_places, k_places, scale):
    scores = jnp.einsum("qshe,kshe->shqk", query, keys, preferred_element_type=jnp.float32) * scale
    allowed = k_places[None, None, None, :] <= q_places[None, None, :, None]
    return (jnp.where(allowed, scores, big_negative), allowed)


def absorb_block(state, query, q_places, k_block, v_block, p_block, scale):
    top, total, summed = state
    scores, allowed = block_scores(query, k_block, q_places, p_block, scale)
    new_top = jnp.maximum(top, jnp.max(scores, axis=-1))
    factor = jnp.exp(top - new_top)
    weights = jnp.where(allowed, jnp.exp(scores - new_top[..., None]), 0.0)
    total = total * factor + jnp.sum(weights, axis=-1)
    update = jnp.einsum(
        "shqk,kshe->qshe", weights.astype(jnp.bfloat16), v_block, preferred_element_type=jnp.float32
    )
    summed = summed * jnp.transpose(factor, (2, 0, 1))[..., None] + update
    return (new_top, total, summed)


def make_absorb(query, q_places, places_all, scale):
    rows, seqs, heads, width = query.shape

    def absorb(carry, piece, start):
        keys, values = piece
        pairs = keys.shape[0] // rows
        k_pairs = keys.reshape(pairs, rows, seqs, heads, width)
        v_pairs = values.reshape(pairs, rows, seqs, heads, width)
        p_pairs = places_all.reshape(pairs, rows)

        def one_pair(state, item):
            k_pair, v_pair, p_pair = item
            return (absorb_block(state, query, q_places, k_pair, v_pair, p_pair, scale), None)

        carry, _ = lax.scan(one_pair, carry, (k_pairs, v_pairs, p_pairs))
        return carry

    return absorb


def grad_block(query, d_mixed, delta, log_total, q_places, k_block, v_block, p_block, scale):
    scores, allowed = block_scores(query, k_block, q_places, p_block, scale)
    weights = jnp.where(allowed, jnp.exp(scores - log_total[..., None]), 0.0)
    d_weights = jnp.einsum("qshe,kshe->shqk", d_mixed, v_block, preferred_element_type=jnp.float32)
    d_scores = (weights * (d_weights - delta[..., None])).astype(jnp.bfloat16)
    part_query = jnp.einsum(
        "shqk,kshe->qshe", d_scores, k_block, preferred_element_type=jnp.float32
    )
    part_key = jnp.einsum("shqk,qshe->kshe", d_scores, query, preferred_element_type=jnp.float32)
    part_value = jnp.einsum(
        "shqk,qshe->kshe", weights.astype(jnp.bfloat16), d_mixed, preferred_element_type=jnp.float32
    )
    return (part_query, part_key, part_value)


def grad_pair(query, d_mixed, delta, log_total, q_places, k_shard, v_shard, p_shard, scale):
    return grad_block(query, d_mixed, delta, log_total, q_places, k_shard, v_shard, p_shard, scale)


def local_ring(
    hidden_in,
    first_values,
    span_table,
    w_query,
    w_key,
    w_value,
    w_out,
    w_up,
    w_down,
    gain_attn,
    shift_attn,
    gain_mlp,
    shift_mlp,
    cotangent,
):
    rows, seqs, width = hidden_in.shape
    count = rows * seqs
    ranks = lax.axis_size("ctx")
    rank = lax.axis_index("ctx")
    span_rows = rows // 2
    local_heads = HEADS // lax.axis_size("tp")
    head_cols = local_heads * HEAD_DIM
    scale = HEAD_DIM ** (-0.5)
    places_all = (
        jnp.repeat(span_table.reshape(-1), span_rows) * span_rows
        + jnp.arange(ranks * rows, dtype=jnp.int32) % span_rows
    )
    q_places = lax.dynamic_slice_in_dim(places_all, rank * rows, rows)
    x_rows = hidden_in.reshape(count, width).astype(jnp.float32)
    unit_one, inverse_one = normalize_rows(x_rows)
    wq_full, wk_full, wv_full, wo_full, gain_one, shift_one = (
        lax.all_gather(w_query, "fsdp", axis=0, tiled=True),
        lax.all_gather(w_key, "fsdp", axis=0, tiled=True),
        lax.all_gather(w_value, "fsdp", axis=0, tiled=True),
        lax.all_gather(w_out, "fsdp", axis=0, tiled=True),
        lax.all_gather(gain_attn, "fsdp", axis=0, tiled=True),
        lax.all_gather(shift_attn, "fsdp", axis=0, tiled=True),
    )
    gain_one = gain_one.astype(jnp.float32)
    h_one = (unit_one * gain_one + shift_one.astype(jnp.float32)).astype(jnp.bfloat16)
    query = jnp.dot(h_one, wq_full, preferred_element_type=jnp.float32).astype(jnp.bfloat16)
    keys = jnp.dot(h_one, wk_full, preferred_element_type=jnp.float32).astype(jnp.bfloat16)
    fresh = jnp.dot(h_one, wv_full, preferred_element_type=jnp.float32).astype(jnp.bfloat16)
    fresh_heads = fresh.reshape(rows, seqs, local_heads // 2, HEAD_DIM)
    reused_heads = first_values.reshape(rows, seqs, local_heads // 2, HEAD_DIM)
    values = jnp.stack([fresh_heads, reused_heads], axis=3).reshape(rows, seqs, head_cols)
    keys_sent = keys.reshape(rows, seqs, head_cols)
    query4 = query.reshape(rows, seqs, local_heads, HEAD_DIM)
    absorb = make_absorb(query4, q_places, places_all, scale)
    start_state = (
        jnp.full((seqs, local_heads, rows), big_negative, jnp.float32),
        jnp.zeros((seqs, local_heads, rows), jnp.float32),
        jnp.zeros((rows, seqs, local_heads, HEAD_DIM), jnp.float32),
    )
    top, total, summed = absorb(
        start_state,
        (
            lax.all_gather(keys_sent, "ctx", axis=0, tiled=True),
            lax.all_gather(values, "ctx", axis=0, tiled=True),
        ),
        jnp.int32(0),
    )
    mixed_exact = summed / jnp.transpose(total, (2, 0, 1))[..., None]
    log_total = top + jnp.log(total)
    mixed = mixed_exact.reshape(count, head_cols).astype(jnp.bfloat16)
    resid = x_rows + lax.psum(contract_cols(mixed, wo_full).astype(jnp.bfloat16), "tp").astype(
        jnp.float32
    )
    unit_two, inverse_two = normalize_rows(resid)
    wu_full, wd_full, gain_two, shift_two = (
        lax.all_gather(w_up, "fsdp", axis=0, tiled=True),
        lax.all_gather(w_down, "fsdp", axis=0, tiled=True),
        lax.all_gather(gain_mlp, "fsdp", axis=0, tiled=True),
        lax.all_gather(shift_mlp, "fsdp", axis=0, tiled=True),
    )
    gain_two = gain_two.astype(jnp.float32)
    h_two = (unit_two * gain_two + shift_two.astype(jnp.float32)).astype(jnp.bfloat16)
    upper = jnp.dot(h_two, wu_full, preferred_element_type=jnp.float32)
    act = gelu_forward(upper).astype(jnp.bfloat16)
    out_rows = resid + lax.psum(contract_cols(act, wd_full).astype(jnp.bfloat16), "tp").astype(
        jnp.float32
    )
    d_out = cotangent.reshape(count, width)
    grad_down = contract_rows(d_out, act)
    d_act = jnp.dot(d_out, wd_full, preferred_element_type=jnp.float32)
    d_upper = (d_act * gelu_slope(upper)).astype(jnp.bfloat16)
    grad_up = contract_rows(h_two, d_upper)
    d_two = lax.psum(contract_cols(d_upper, wu_full).astype(jnp.bfloat16), "tp").astype(jnp.float32)
    grad_gain_mlp = jnp.sum(d_two * unit_two, axis=0)
    grad_shift_mlp = jnp.sum(d_two, axis=0)
    d_resid = d_out.astype(jnp.float32) + normalize_back(d_two, unit_two, inverse_two, gain_two)
    d_branch = d_resid.astype(jnp.bfloat16)
    grad_outproj = contract_rows(d_branch, mixed)
    d_mixed = jnp.dot(d_branch, wo_full, preferred_element_type=jnp.float32).astype(jnp.bfloat16)
    d_mixed4 = d_mixed.reshape(rows, seqs, local_heads, HEAD_DIM)
    delta = jnp.transpose(jnp.sum(d_mixed4.astype(jnp.float32) * mixed_exact, axis=-1), (1, 2, 0))
    zero_query = jnp.zeros((rows, seqs, local_heads, HEAD_DIM), jnp.float32)
    zero_keys = jnp.zeros((rows, seqs, head_cols), jnp.float32)

    def visit(step, state):
        moving_k, moving_v, acc_k, acc_v, acc_q = state
        source = (rank - step) % ranks
        p_block = lax.dynamic_slice_in_dim(places_all, source * rows, rows)
        part_q, part_k, part_v = grad_pair(
            query4,
            d_mixed4,
            delta,
            log_total,
            q_places,
            moving_k.reshape(rows, seqs, local_heads, HEAD_DIM),
            moving_v.reshape(rows, seqs, local_heads, HEAD_DIM),
            p_block,
            scale,
        )
        acc_k = acc_k + part_k.reshape(rows, seqs, head_cols)
        acc_v = acc_v + part_v.reshape(rows, seqs, head_cols)
        moving_k, moving_v = passed_along((moving_k, moving_v), "ctx", 1)
        acc_k, acc_v = (
            passed_along(acc_k.astype(jnp.bfloat16), "ctx", 1).astype(acc_k.dtype),
            passed_along(acc_v.astype(jnp.bfloat16), "ctx", 1).astype(acc_v.dtype),
        )
        return (moving_k, moving_v, acc_k, acc_v, acc_q + part_q)

    final_state = lax.fori_loop(
        0, ranks, visit, (keys_sent, values, zero_keys, zero_keys, zero_query)
    )
    d_keys = final_state[2]
    d_values = final_state[3]
    d_query = final_state[4]
    d_query_low = (d_query * scale).reshape(count, head_cols).astype(jnp.bfloat16)
    d_keys_low = (d_keys * scale).reshape(count, head_cols).astype(jnp.bfloat16)
    split_values = d_values.reshape(rows, seqs, local_heads // 2, 2, HEAD_DIM)
    d_fresh = split_values[:, :, :, 0, :].reshape(count, head_cols // 2).astype(jnp.bfloat16)
    grad_first = split_values[:, :, :, 1, :].reshape(rows, seqs, head_cols // 2)
    grad_query = contract_rows(h_one, d_query_low)
    grad_key = contract_rows(h_one, d_keys_low)
    grad_value = contract_rows(h_one, d_fresh)
    d_part = (
        contract_cols(d_query_low, wq_full)
        + contract_cols(d_keys_low, wk_full)
        + contract_cols(d_fresh, wv_full)
    )
    d_one = lax.psum(d_part.astype(jnp.bfloat16), "tp").astype(jnp.float32)
    grad_gain_attn = jnp.sum(d_one * unit_one, axis=0)
    grad_shift_attn = jnp.sum(d_one, axis=0)
    d_input = d_resid + normalize_back(d_one, unit_one, inverse_one, gain_one)
    shared = (
        lax.psum_scatter(
            grad_query.astype(jnp.bfloat16), "fsdp", scatter_dimension=0, tiled=True
        ).astype(jnp.float32),
        lax.psum_scatter(
            grad_key.astype(jnp.bfloat16), "fsdp", scatter_dimension=0, tiled=True
        ).astype(jnp.float32),
        lax.psum_scatter(
            grad_value.astype(jnp.bfloat16), "fsdp", scatter_dimension=0, tiled=True
        ).astype(jnp.float32),
        lax.psum_scatter(
            grad_outproj.astype(jnp.bfloat16), "fsdp", scatter_dimension=0, tiled=True
        ).astype(jnp.float32),
        lax.psum_scatter(
            grad_up.astype(jnp.bfloat16), "fsdp", scatter_dimension=0, tiled=True
        ).astype(jnp.float32),
        lax.psum_scatter(
            grad_down.astype(jnp.bfloat16), "fsdp", scatter_dimension=0, tiled=True
        ).astype(jnp.float32),
        lax.psum_scatter(
            grad_gain_attn.astype(jnp.bfloat16), "fsdp", scatter_dimension=0, tiled=True
        ).astype(jnp.float32),
        lax.psum_scatter(
            grad_shift_attn.astype(jnp.bfloat16), "fsdp", scatter_dimension=0, tiled=True
        ).astype(jnp.float32),
        lax.psum_scatter(
            grad_gain_mlp.astype(jnp.bfloat16), "fsdp", scatter_dimension=0, tiled=True
        ).astype(jnp.float32),
        lax.psum_scatter(
            grad_shift_mlp.astype(jnp.bfloat16), "fsdp", scatter_dimension=0, tiled=True
        ).astype(jnp.float32),
    )
    summed_grads = (
        lax.psum(shared[0].astype(jnp.bfloat16), "ctx").astype(jnp.float32),
        lax.psum(shared[1].astype(jnp.bfloat16), "ctx").astype(jnp.float32),
        lax.psum(shared[2].astype(jnp.bfloat16), "ctx").astype(jnp.float32),
        lax.psum(shared[3].astype(jnp.bfloat16), "ctx").astype(jnp.float32),
        lax.psum(shared[4].astype(jnp.bfloat16), "ctx").astype(jnp.float32),
        lax.psum(shared[5].astype(jnp.bfloat16), "ctx").astype(jnp.float32),
        lax.psum(shared[6].astype(jnp.bfloat16), "ctx").astype(jnp.float32),
        lax.psum(shared[7].astype(jnp.bfloat16), "ctx").astype(jnp.float32),
        lax.psum(shared[8].astype(jnp.bfloat16), "ctx").astype(jnp.float32),
        lax.psum(shared[9].astype(jnp.bfloat16), "ctx").astype(jnp.float32),
    )
    return (
        out_rows.reshape(rows, seqs, width),
        d_input.reshape(rows, seqs, width),
        grad_first,
        summed_grads[0],
        summed_grads[1],
        summed_grads[2],
        summed_grads[3],
        summed_grads[4],
        summed_grads[5],
        summed_grads[6],
        summed_grads[7],
        summed_grads[8],
        summed_grads[9],
    )


def swap_fsdp(value, flip):
    count = lax.axis_size("fsdp")
    return lax.ppermute(value, "fsdp", [(i, i ^ flip) for i in range(count)])


def swap_tp(value):
    return lax.ppermute(value, "tp", [(0, 1), (1, 0)])


def swap_ctx(value):
    return lax.ppermute(value, "ctx", [(0, 1), (1, 0)])


def after(value, *others):
    return lax.optimization_barrier((value, others))[0]


def gather_columns(shard):
    return [shard] + [swap_fsdp(shard, 2 * k) for k in range(1, lax.axis_size("fsdp") // 2)]


def gather_pairs(near):
    return [block for mine in near for block in (mine, swap_fsdp(mine, 1))]


def matmul(left, right, left_dim, right_dim):
    return lax.dot_general(left, right, (((left_dim,), (right_dim,)), ((), ())), preferred_element_type=wide)


def shapes(*pairs):
    return tuple(jax.ShapeDtypeStruct(shape, dtype) for shape, dtype in pairs)


def parity_heads(block, odd):
    count = block.shape[1] // HEAD_DIM
    return jnp.concatenate([block[:, j * HEAD_DIM : (j + 1) * HEAD_DIM] for j in range(odd, count, 2)], axis=1)


def woven_heads(even, odd):
    count = even.shape[1] // HEAD_DIM
    parts = []
    for i in range(count):
        parts += [even[:, i * HEAD_DIM : (i + 1) * HEAD_DIM], odd[:, i * HEAD_DIM : (i + 1) * HEAD_DIM]]
    return jnp.concatenate(parts, axis=1)


def pack_attn_kernel(wq, wk, wv, g0, g1, g2, g3, out):
    rank = lax.axis_index("ctx")
    shard = wq.shape[0]

    def pick(ref):
        block = ref[...].astype(wide)
        return jnp.where(rank == 0, parity_heads(block, 0), parity_heads(block, 1))

    gains = jnp.concatenate([g[...].astype(wide) for g in (g0, g1, g2, g3)] + [jnp.zeros((4, shard), wide)], axis=0)
    gains = jnp.concatenate([gains, jnp.zeros((8, 128 - shard), wide)], axis=1).T[:shard]
    pad = jnp.zeros((shard, HEAD_DIM - 8), wide)
    out[...] = jnp.concatenate([pick(wq), pick(wk), wv[...].astype(wide), gains, pad], axis=1).astype(low)


def pack_late_kernel(wo, wu, wd, out):
    rank = lax.axis_index("ctx")
    cols, units = wo.shape[1], wu.shape[1] // 2
    block = wo[...].astype(wide)
    even, odd = parity_heads(block, 0), parity_heads(block, 1)
    own = jnp.where(rank == 0, even, odd)
    other = jnp.where(rank == 0, odd, even)
    out[:, :cols] = jnp.concatenate([own, other], axis=1).astype(low)
    out[:, cols : cols + units] = jnp.where(rank == 0, wu[:, :units], wu[:, units:])
    out[:, cols + units :] = jnp.where(rank == 0, wd[:, :units], wd[:, units:])


def place_blocks(blocks, store):
    me = lax.axis_index("fsdp")
    for m, block in enumerate(blocks):
        rows = block.shape[0]
        store(pl.ds(pl.multiple_of((me ^ m) * rows, 32), rows), block)


def row_norm(values):
    mean = jnp.mean(values, axis=-1, keepdims=True)
    centred = values - mean
    inverse = lax.rsqrt(jnp.mean(centred * centred, axis=-1, keepdims=True) + eps_norm)
    return centred * inverse, inverse


def quarter_of_place(table):
    rank, side = lax.axis_index("ctx"), lax.axis_index("tp")
    held = [table[rank ^ (q // 2), side ^ (q % 2)] for q in range(4)]
    return [sum(jnp.where(held[q] == p, q, 0) for q in range(4)) for p in range(4)]


def attn_kernel(table, hid, pair, pair2, b0, b1, b2, b3, b4, b5, b6, b7, first, first_far,
                x_out, h_out, w_out, gains_out, qkv_out, mix_out, low_out, lse_out, keys_scr):
    rank, side = lax.axis_index("ctx"), lax.axis_index("tp")
    span = pair.shape[1]
    cols = first.shape[0]
    heads = cols // HEAD_DIM

    def store(where, block):
        w_out[where, :] = block[...]

    place_blocks((b0, b1, b2, b3, b4, b5, b6, b7), store)
    gains = w_out[:, 512:640].astype(wide).T[64:72]
    gains_out[...] = gains
    gain, shift = gains[0:1], gains[1:2]
    x_out[0] = hid[pl.ds(pl.multiple_of(side * span, span), span), :]
    x_out[1] = hid[pl.ds(pl.multiple_of((1 - side) * span, span), span), :]
    x_out[2] = pair[0]
    x_out[3] = pair2[0]
    step = 64

    def norm_chunk(i, carry):
        for q in range(4):
            where = pl.ds(pl.multiple_of(i * step, step), step)
            unit, _ = row_norm(x_out[q, where, :].astype(wide))
            h_out[q, where, :] = (unit * gain + shift).astype(low)
        return carry

    lax.fori_loop(0, span // step, norm_chunk, 0)
    w_turned = w_out[:, : 3 * cols].T
    for q in range(4):
        qkv_out[q] = matmul(w_turned, h_out[q], 1, 1).astype(low)

    @pl.when(rank == 1)
    def _():
        for q in range(4):
            ref = first if q < 2 else first_far
            half = side if q % 2 == 0 else 1 - side
            qkv_out[q, 2 * cols :, :] = jnp.where(half == 0, ref[:, :span], ref[:, span:])

    order = quarter_of_place(table)
    below = lax.broadcasted_iota(jnp.int32, (span, span), 0) <= lax.broadcasted_iota(jnp.int32, (span, span), 1)
    lse_out[...] = jnp.zeros_like(lse_out)

    for h in range(heads):
        base = h * HEAD_DIM
        for p in range(4):
            keys_scr[p] = qkv_out[order[p], cols + base : cols + base + HEAD_DIM, :].T
        for qp in range(4):
            query = qkv_out[order[qp], base : base + HEAD_DIM, :] * low(HEAD_DIM ** -0.5)
            scores = [matmul(keys_scr[kp], query, 1, 0) for kp in range(qp + 1)]
            scores[qp] = jnp.where(below, scores[qp], big_negative)
            top = jnp.max(scores[0], axis=0, keepdims=True)
            for s in scores[1:]:
                top = jnp.maximum(top, jnp.max(s, axis=0, keepdims=True))
            total = jnp.zeros((1, span), wide)
            mixed = jnp.zeros((HEAD_DIM, span), wide)
            for kp in range(qp + 1):
                weights = jnp.exp(scores[kp] - top)
                total = total + jnp.sum(weights, axis=0, keepdims=True)
                value = qkv_out[order[kp], 2 * cols + base : 2 * cols + base + HEAD_DIM, :]
                mixed = mixed + matmul(value, weights.astype(low), 1, 0)
            mixed = mixed / total
            mix_out[order[qp], base : base + HEAD_DIM, :] = mixed
            low_out[order[qp], base : base + HEAD_DIM, :] = mixed.astype(low)
            lse_out[order[qp], h : h + 1, :] = top + jnp.log(total)


def place_late_kernel(b0, b1, b2, b3, b4, b5, b6, b7, cot, pair, pair2, wo_out, wu_out, wd_out, cot_out):
    side = lax.axis_index("tp")
    span = pair.shape[1]
    cols, units = wo_out.shape[1], wu_out.shape[1]

    def store(where, block):
        wo_out[where, :] = block[:, :cols]
        wu_out[where, :] = block[:, cols : cols + units]
        wd_out[where, :] = block[:, cols + units :]

    place_blocks((b0, b1, b2, b3, b4, b5, b6, b7), store)
    cot_out[0] = cot[pl.ds(pl.multiple_of(side * span, span), span), :]
    cot_out[1] = cot[pl.ds(pl.multiple_of((1 - side) * span, span), span), :]
    cot_out[2] = pair[1]
    cot_out[3] = pair2[1]


def mlp_kernel(x, mix0, mix1, mix2, mix3, wo_own, wo_side, wu, wd, gains, cot,
               resid_out, act_out, h_out, dup_out, keep_out, send_out):
    q = pl.program_id(0)
    mixed = jnp.concatenate([mix0[0], mix1[0], mix2[0], mix3[0]], axis=0).T
    half = wo_own.shape[1]
    proj = matmul(mixed[:, :half], wo_own[...], 1, 1) + matmul(mixed[:, half:], wo_side[...], 1, 1)
    resid = x[0].astype(wide) + proj

    @pl.when(q < 2)
    def _():
        resid_out[0] = resid

    unit, _ = row_norm(resid)
    h_two = (unit * gains[2:3, :] + gains[3:4, :]).astype(low)
    h_out[0] = h_two
    upper = matmul(h_two, wu[...], 1, 0)
    square = upper * upper
    tanh = jnp.tanh(gelu_coef * upper * (1.0 + cube_coef * square))
    act_out[0] = (0.5 * upper * (1.0 + tanh)).astype(low)
    slope = 0.5 * (1.0 + tanh) + 0.5 * upper * (1.0 - tanh * tanh) * gelu_coef * (1.0 + 3.0 * cube_coef * square)
    d_act = matmul(cot[0], wd[...], 1, 0)
    d_upper = (d_act * slope).astype(low)
    dup_out[0] = d_upper
    part = matmul(d_upper, wu[...], 1, 1).astype(low)

    @pl.when(q % 2 == 0)
    def _():
        keep_out[0] = part

    @pl.when(q % 2 == 1)
    def _():
        send_out[0] = part


def scatter_slots(value, keep, send, lanes):
    me = lax.axis_index("fsdp")
    rows = keep.shape[1]
    for k in range(keep.shape[0]):
        base = (me >> 1) ^ k
        keep[k, :, lanes] = value[pl.ds(pl.multiple_of((base * 2 + (me & 1)) * rows, 32), rows), :].astype(low)
        send[k, :, lanes] = value[pl.ds(pl.multiple_of((base * 2 + ((me & 1) ^ 1)) * rows, 32), rows), :].astype(low)


def mlp_grad_kernel(cot, act, h_two, d_upper, wd, keep_out, send_out, out_keep, out_send, grad):
    units = act.shape[2]
    width = cot.shape[2]
    for left, right, first in ((h_two, d_upper, 0), (cot, act, units)):
        total = matmul(left[0], right[0], 0, 0)
        for q in range(1, 4):
            total = total + matmul(left[q], right[q], 0, 0)
        grad[...] = total
        scatter_slots(grad, keep_out, send_out, slice(first, first + units))
    for q in range(4):
        part = matmul(act[q], wd[...], 1, 1).astype(low)
        (out_keep if q % 2 == 0 else out_send)[q // 2] = part


def norm_back(d_norm, unit, inverse, gain):
    scaled = d_norm * gain
    inner = scaled - jnp.mean(scaled, axis=-1, keepdims=True) - unit * jnp.mean(scaled * unit, axis=-1, keepdims=True)
    return inverse * inner


def branch_kernel(keep, got, far, resid, cot, gains, d_resid_out, low_out, sums_out):
    d_two = keep[0].astype(wide) + got[0].astype(wide) + far[...].astype(wide)
    unit, inverse = row_norm(resid[0])
    sums_out[...] = jnp.zeros_like(sums_out)
    sums_out[0:1, :] = jnp.sum(d_two * unit, axis=0, keepdims=True)
    sums_out[1:2, :] = jnp.sum(d_two, axis=0, keepdims=True)
    d_resid = cot[0].astype(wide) + norm_back(d_two, unit, inverse, gains[2:3, :])
    d_resid_out[...] = d_resid
    low_out[...] = d_resid.astype(low)


def attn_back_kernel(table, br0, br1, br2, br3, wo, qkv, mix, lse, d_out, d_first,
                     dm_scr, keys_scr, values_scr, dq_scr):
    rank = lax.axis_index("ctx")
    span = qkv.shape[2]
    cols = mix.shape[1]
    heads = cols // HEAD_DIM
    wo_turned = wo[:, :cols].T
    branches = (br0, br1, br2, br3)
    for q in range(4):
        dm_scr[q] = matmul(wo_turned, branches[q][...], 1, 1).astype(low)
    order = quarter_of_place(table)
    below = lax.broadcasted_iota(jnp.int32, (span, span), 0) <= lax.broadcasted_iota(jnp.int32, (span, span), 1)
    root = low(HEAD_DIM ** -0.5)
    for h in range(heads):
        base = h * HEAD_DIM
        mine = slice(base, base + HEAD_DIM)
        delta = []
        for p in range(4):
            keys_scr[p] = qkv[order[p], cols + base : cols + base + HEAD_DIM, :].T
            values_scr[p] = qkv[order[p], 2 * cols + base : 2 * cols + base + HEAD_DIM, :].T
            delta.append(jnp.sum(dm_scr[order[p], mine, :].astype(wide) * mix[order[p], mine, :], axis=0, keepdims=True))
        for kp in range(4):
            d_key = jnp.zeros((HEAD_DIM, span), wide)
            d_value = jnp.zeros((HEAD_DIM, span), wide)
            key = qkv[order[kp], cols + base : cols + base + HEAD_DIM, :]
            for qp in range(kp, 4):
                query = qkv[order[qp], mine, :] * root
                d_mixed = dm_scr[order[qp], mine, :]
                weights = jnp.exp(matmul(keys_scr[kp], query, 1, 0) - lse[order[qp], h : h + 1, :])
                if kp == qp:
                    weights = jnp.where(below, weights, 0.0)
                d_weights = matmul(values_scr[kp], d_mixed, 1, 0)
                d_scores = (weights * (d_weights - delta[qp])).astype(low)
                d_value = d_value + matmul(d_mixed, weights.astype(low), 1, 1)
                d_key = d_key + matmul(query, d_scores, 1, 1)
                d_query = matmul(key, d_scores, 1, 0)
                dq_scr[qp] = d_query if kp == 0 else dq_scr[qp] + d_query
            d_out[order[kp], cols + base : cols + base + HEAD_DIM, :] = d_key.astype(low)
            d_first[order[kp], mine, :] = d_value
            d_out[order[kp], 2 * cols + base : 2 * cols + base + HEAD_DIM, :] = jnp.where(rank == 0, d_value, 0.0).astype(low)
        for qp in range(4):
            d_out[order[qp], mine, :] = (dq_scr[qp] * HEAD_DIM ** -0.5).astype(low)


def d_one_kernel(d_qkv, w, x, sums_two, keep_out, send_out, sums_out):
    q = pl.program_id(0)
    wide_cols = d_qkv.shape[1]
    part = matmul(d_qkv[0].T, w[:, :wide_cols], 1, 1)
    unit, _ = row_norm(x[0].astype(wide))

    @pl.when(q == 0)
    def _():
        sums_out[...] = jnp.concatenate([jnp.zeros_like(sums_two), sums_two[...]], axis=0)[6:14]

    sums_out[0:1, :] += jnp.sum(part * unit, axis=0, keepdims=True)
    sums_out[1:2, :] += jnp.sum(part, axis=0, keepdims=True)

    @pl.when(q % 2 == 0)
    def _():
        keep_out[0] = part.astype(low)

    @pl.when(q % 2 == 1)
    def _():
        send_out[0] = part.astype(low)


def attn_grad_kernel(d_qkv, h_one, keep_out, send_out, grad):
    turned = matmul(d_qkv[0], h_one[0], 1, 0)
    for q in range(1, 4):
        turned = turned + matmul(d_qkv[q], h_one[q], 1, 0)
    grad[...] = turned.T
    scatter_slots(grad, keep_out, send_out, slice(None))


def proj_grad_kernel(low_mix, br0, br1, br2, br3, sums, sums_side, keep_out, send_out, grad):
    cols = low_mix.shape[1]
    turned = matmul(low_mix[0], br0[...], 1, 0)
    for q, branch in ((1, br1), (2, br2), (3, br3)):
        turned = turned + matmul(low_mix[q], branch[...], 1, 0)
    gains = sums[...] + sums_side[...].astype(wide)
    pad = jnp.zeros((HEAD_DIM - gains.shape[0], gains.shape[1]), wide)
    grad[...] = jnp.concatenate([turned, gains, pad], axis=0).T
    scatter_slots(grad, keep_out, send_out, slice(None))


def pair_kernel(keep, got, *outs):
    for k, out in enumerate(outs):
        out[...] = (keep[k].astype(wide) + got[k].astype(wide)).astype(low)


def add(*parts):
    return sum(part.astype(wide) for part in parts).astype(low)


def scatter_over(keep, got):
    shape = keep.shape[1:]
    parts = pl.pallas_call(pair_kernel, out_shape=shapes(*[(shape, low)] * keep.shape[0]))(keep, got)
    return add(parts[0], *[swap_fsdp(parts[k], 2 * k) for k in range(1, keep.shape[0])])


def finish_mlp_kernel(own, far, up_out, down_out):
    rank = lax.axis_index("ctx")
    units = own.shape[1] // 2
    a, b = own[...].astype(wide), far[...].astype(wide)
    lower, upper = jnp.where(rank == 0, a, b), jnp.where(rank == 0, b, a)
    up_out[:, :units] = lower[:, :units]
    up_out[:, units:] = upper[:, :units]
    down_out[:, :units] = lower[:, units:]
    down_out[:, units:] = upper[:, units:]


def finish_attn_kernel(own, far, own_proj, far_proj, q_out, k_out, v_out, o_out, g0, g1, g2, g3):
    rank = lax.axis_index("ctx")
    cols = v_out.shape[1]
    rows = own.shape[0]
    a, b = own[...].astype(wide), far[...].astype(wide)
    even, odd = jnp.where(rank == 0, a, b), jnp.where(rank == 0, b, a)
    q_out[...] = woven_heads(even[:, :cols], odd[:, :cols])
    k_out[...] = woven_heads(even[:, cols : 2 * cols], odd[:, cols : 2 * cols])
    v_out[...] = even[:, 2 * cols : 3 * cols]
    c, d = own_proj[...].astype(wide), far_proj[...].astype(wide)
    even, odd = jnp.where(rank == 0, c, d), jnp.where(rank == 0, d, c)
    o_out[...] = woven_heads(even[:, :cols], odd[:, :cols])
    both = c[:, 128:256] + d[:, 128:256]
    gains = jnp.concatenate([both, jnp.zeros((128 - rows, 128), wide)], axis=0).T
    for i, out in enumerate((g0, g1, g2, g3)):
        out[...] = gains[64 + i : 65 + i, :rows]


def store_rows(out, first, value):
    pieces = value.shape[1] // 128
    for j in range(pieces):
        out[pl.ds(first * pieces + j, value.shape[0], stride=pieces), :] = value[:, j * 128 : (j + 1) * 128]


def out_kernel(resid, own, beside, out):
    side = lax.axis_index("tp")
    span = own.shape[0]
    store_rows(out, side * span, resid[0] + own[...].astype(wide))
    store_rows(out, (1 - side) * span, resid[1] + beside[...].astype(wide))


def input_grad_kernel(x, own, beside, d_own, d_beside, gains, out):
    side = lax.axis_index("tp")
    span = own.shape[0]
    for k, (d_one, d_resid) in enumerate(((own, d_own), (beside, d_beside))):
        unit, inverse = row_norm(x[k].astype(wide))
        value = d_resid[...] + norm_back(d_one[...].astype(wide), unit, inverse, gains[0:1, :])
        store_rows(out, (side if k == 0 else 1 - side) * span, value)


def first_grad_kernel(d_first, far, out):
    rank, side = lax.axis_index("ctx"), lax.axis_index("tp")
    span = d_first.shape[2]

    @pl.when(rank == 0)
    def _():
        out[...] = far[...].astype(wide)

    @pl.when(rank == 1)
    def _():
        out[:, :span] = jnp.where(side == 0, d_first[0], d_first[1])
        out[:, span:] = jnp.where(side == 0, d_first[1], d_first[0])


def first_send_kernel(d_first, out):
    side = lax.axis_index("tp")
    span = d_first.shape[2]
    out[:, :span] = jnp.where(side == 0, d_first[2], d_first[3]).astype(low)
    out[:, span:] = jnp.where(side == 0, d_first[3], d_first[2]).astype(low)


def local_split(
    hidden_in,
    first_values,
    span_table,
    w_query,
    w_key,
    w_value,
    w_out,
    w_up,
    w_down,
    gain_attn,
    shift_attn,
    gain_mlp,
    shift_mlp,
    cotangent,
):
    rows, seqs, width = hidden_in.shape
    span = rows // 2
    shard = w_query.shape[0]
    cols = w_query.shape[1] // 2
    units = w_up.shape[1] // 2
    pairs = lax.axis_size("fsdp") // 2
    smem = pl.BlockSpec(memory_space=pltpu.SMEM)
    vmem = pl.BlockSpec(memory_space=pltpu.VMEM)
    side = lax.axis_index("tp")

    def quarter_spec(c, turn=lambda q: q, s=span):
        return pl.BlockSpec((1, s, c), lambda q: (turn(q), 0, 0))

    def whole_spec(*shape):
        return pl.BlockSpec(shape, lambda q: (0,) * len(shape))

    hidden = hidden_in.reshape(rows, width)
    cot = cotangent.reshape(rows, width)
    first = first_values.reshape(rows, cols).T

    own_pair = jnp.stack([lax.dynamic_slice_in_dim(block, side * span, span) for block in (hidden, cot)])
    gains_in = [g.reshape(1, shard) for g in (gain_attn, shift_attn, gain_mlp, shift_mlp)]
    attn_shard = pl.pallas_call(pack_attn_kernel, out_shape=jax.ShapeDtypeStruct((shard, 640), low))(
        w_query, w_key, w_value, *gains_in
    )
    pair = swap_ctx(after(own_pair, attn_shard))
    near = gather_columns(attn_shard)
    attn_blocks = gather_pairs(near)
    w_late = after((w_out, w_up, w_down), attn_shard)
    late_shard = pl.pallas_call(
        pack_late_kernel, out_shape=jax.ShapeDtypeStruct((shard, 2 * cols + 2 * units), low)
    )(*w_late)
    late_near = gather_columns(late_shard)
    first_far = lax.ppermute(first, "ctx", [(0, 1)])
    pair2 = swap_tp(after(pair, *attn_blocks))

    x4, h_one, w_qkv, gains, qkv, mix, low_mix, lse = pl.pallas_call(
        attn_kernel,
        in_specs=[smem] + [vmem] * 13,
        out_shape=shapes(
            ((4, span, width), low), ((4, span, width), low), ((width, 640), low), ((8, width), wide),
            ((4, 3 * cols, span), low), ((4, cols, span), wide), ((4, cols, span), low), ((4, 8, span), wide),
        ),
        scratch_shapes=[pltpu.VMEM((4, span, HEAD_DIM), low)],
    )(span_table, hidden, pair, pair2, *attn_blocks, first, first_far)

    mix_far = swap_ctx(low_mix)
    mix_side = swap_tp(low_mix)
    late_blocks = gather_pairs([late_near[0]] + [after(block, lse) for block in late_near[1:]])
    wo_half, wu, wd, cot4 = pl.pallas_call(
        place_late_kernel,
        out_shape=shapes(((width, 2 * cols), low), ((width, units), low), ((width, units), low), ((4, span, width), low)),
    )(*late_blocks, cot, pair, pair2)
    wo_side = swap_tp(wo_half)
    mix_side_far = swap_tp(mix_far)

    half_spec = pl.BlockSpec((1, span, width), lambda q: (q // 2, 0, 0))
    resid, act, h_two, d_upper, two_keep, two_send = pl.pallas_call(
        mlp_kernel,
        grid=(4,),
        in_specs=[
            quarter_spec(width),
            quarter_spec(span, s=cols),
            quarter_spec(span, lambda q: (q + 2) % 4, cols),
            quarter_spec(span, lambda q: q + 1 - 2 * (q % 2), cols),
            quarter_spec(span, lambda q: 3 - q, cols),
            whole_spec(width, 2 * cols),
            whole_spec(width, 2 * cols),
            whole_spec(width, units),
            whole_spec(width, units),
            whole_spec(8, width),
            quarter_spec(width),
        ],
        out_specs=[
            quarter_spec(width, lambda q: jnp.minimum(q, 1)),
            quarter_spec(units),
            quarter_spec(width),
            quarter_spec(units),
            half_spec,
            half_spec,
        ],
        out_shape=shapes(
            ((2, span, width), wide), ((4, span, units), low), ((4, span, width), low), ((4, span, units), low),
            ((2, span, width), low), ((2, span, width), low),
        ),
    )(x4, low_mix, mix_far, mix_side, mix_side_far, wo_half, wo_side, wu, wd, gains, cot4)

    two_got = swap_tp(two_send)
    two_far = swap_ctx(add(two_keep[1], two_got[1]))
    mlp_keep, mlp_send, out_keep, out_send = pl.pallas_call(
        mlp_grad_kernel,
        out_shape=shapes(
            ((pairs, shard, 2 * units), low), ((pairs, shard, 2 * units), low), ((2, span, width), low), ((2, span, width), low)
        ),
        scratch_shapes=[pltpu.VMEM((width, units), wide)],
    )(cot4, act, h_two, d_upper, wd)
    d_resid, branch, sums_two = pl.pallas_call(
        branch_kernel,
        out_shape=shapes(((span, width), wide), ((span, width), low), ((8, width), wide)),
    )(two_keep, two_got, after(two_far, mlp_keep), resid, cot4, gains)
    branch_far = swap_ctx(branch)
    branch_side = swap_tp(branch)
    d_resid_beside = swap_tp(d_resid)
    branch_side_far = swap_tp(branch_far)
    branches = (branch, branch_side, branch_far, branch_side_far)

    flat = jax.ShapeDtypeStruct((rows * width // 128, 128), wide)
    out_got = swap_tp(out_send)
    out_half = add(out_keep[1], out_got[1])
    out_far = swap_ctx(out_half)
    out_sum = add(out_keep[0], out_got[0], out_far)
    out_rows = pl.pallas_call(out_kernel, out_shape=flat)(resid, out_sum, swap_tp(out_sum))
    mlp_total = scatter_over(mlp_keep, swap_fsdp(mlp_send, 1))

    d_qkv, d_first = pl.pallas_call(
        attn_back_kernel,
        in_specs=[smem] + [vmem] * 8,
        out_shape=shapes(((4, 3 * cols, span), low), ((4, cols, span), wide)),
        scratch_shapes=[
            pltpu.VMEM((4, cols, span), low),
            pltpu.VMEM((4, span, HEAD_DIM), low),
            pltpu.VMEM((4, span, HEAD_DIM), low),
            pltpu.VMEM((4, HEAD_DIM, span), wide),
        ],
    )(span_table, *branches, after(wo_half, out_half), qkv, mix, lse)

    last_keep, last_send = pl.pallas_call(
        attn_grad_kernel,
        out_shape=shapes(((pairs, shard, 3 * cols), low), ((pairs, shard, 3 * cols), low)),
        scratch_shapes=[pltpu.VMEM((width, 3 * cols), wide)],
    )(d_qkv, h_one)
    one_keep, one_send, sums = pl.pallas_call(
        d_one_kernel,
        grid=(4,),
        in_specs=[quarter_spec(span, s=3 * cols), whole_spec(width, 640), quarter_spec(width), whole_spec(8, width)],
        out_specs=[half_spec, half_spec, whole_spec(8, width)],
        out_shape=shapes(((2, span, width), low), ((2, span, width), low), ((8, width), wide)),
    )(after(d_qkv, last_send), w_qkv, x4, sums_two)
    one_got = swap_tp(one_send)
    sums_side = swap_tp(sums.astype(low))
    one_far = swap_ctx(add(one_keep[1], one_got[1]))
    last_got = swap_fsdp(last_send, 1)
    last_total = scatter_over(last_keep, last_got)
    proj_keep, proj_send = pl.pallas_call(
        proj_grad_kernel,
        out_shape=shapes(((pairs, shard, 256), low), ((pairs, shard, 256), low)),
        scratch_shapes=[pltpu.VMEM((width, 256), wide)],
    )(after(low_mix, last_got), *branches, sums, sums_side)
    proj_total = scatter_over(proj_keep, swap_fsdp(proj_send, 1))

    one_sum = add(one_keep[0], one_got[0], one_far)
    d_input = pl.pallas_call(input_grad_kernel, out_shape=flat)(
        x4, one_sum, swap_tp(one_sum), d_resid, d_resid_beside, gains
    )

    first_sent = pl.pallas_call(first_send_kernel, out_shape=jax.ShapeDtypeStruct((cols, rows), low))(d_first)
    grad_first = pl.pallas_call(first_grad_kernel, out_shape=jax.ShapeDtypeStruct((cols, rows), wide))(
        d_first, lax.ppermute(first_sent, "ctx", [(1, 0)])
    )

    grad_up, grad_down = pl.pallas_call(finish_mlp_kernel, out_shape=shapes(*[((shard, 2 * units), wide)] * 2))(
        mlp_total, swap_ctx(mlp_total)
    )
    grads = pl.pallas_call(
        finish_attn_kernel,
        out_shape=shapes(
            ((shard, 2 * cols), wide), ((shard, 2 * cols), wide), ((shard, cols), wide), ((shard, 2 * cols), wide),
            *[((1, shard), wide)] * 4,
        ),
    )(last_total, swap_ctx(last_total), proj_total, swap_ctx(proj_total))
    return (
        out_rows.reshape(rows, seqs, width),
        d_input.reshape(rows, seqs, width),
        grad_first.T.reshape(rows, seqs, cols),
        grads[0],
        grads[1],
        grads[2],
        grads[3],
        grad_up,
        grad_down,
        *[g.reshape(shard) for g in grads[4:]],
    )


def solution(mesh):
    local = local_split if mesh.shape["ctx"] == 2 and mesh.shape["tp"] == 2 else local_ring
    rows, heads, wide_rows = P("ctx", "fsdp", None), P("ctx", "fsdp", "tp"), P("fsdp", "tp")
    return jax.shard_map(
        local,
        mesh=mesh,
        in_specs=(rows, heads, P()) + (wide_rows,) * 6 + (P("fsdp"),) * 4 + (rows,),
        out_specs=(rows, rows, heads) + (wide_rows,) * 6 + (P("fsdp"),) * 4,
        check_vma=False,
    )
```
